128 devices in a mesh: field: 4 (over x_hi, core), slab: 32 (over x_lo, z, y).
Axes of the slice: x: 4 (x_hi: 2, x_lo: 2; x = x_hi * 2 + x_lo), y: 4, z: 4, core: 2. Of those that a mesh axis runs over, the one named last changes fastest.
Arguments:
- velocity_u: float32 [512, 512, 512], P('field', 'slab'), may hold values from -6 to 6
- velocity_v: float32 [512, 512, 512], P('field', 'slab'), may hold values from -6 to 6
- scalar_theta: float32 [512, 512, 512], P('field', 'slab'), may hold values from -6 to 6
Outputs:
- spectrum: float32 [4, 320, 320, 320], P('field', 'slab')
The draws below stay inside these ranges and needn't reach their ends.
All inputs are finite; a program needn't handle non-finite values.
Results may differ from the reference program's by a relative error of at most 0.00029.
Values sent between devices are 32-bit elements; how exact they have to be, the bound alone decides.
A program may use at most 128 MiB of HBM per device.

```python
import jax
import jax.numpy as jnp

N = 512
KEEP = 160


def levels(own_key, shape, cuts, smallest, largest):
    factor_of, own = 1.0, jax.random.fold_in(own_key, 6)
    for axis_at, parts in cuts:
        draws = jnp.exp(jax.random.uniform(jax.random.fold_in(own, axis_at), (parts,), jnp.float32, smallest / len(cuts), largest / len(cuts)))
        factor_of = factor_of * jnp.repeat(draws, shape[axis_at] // parts).reshape([-1 if axis == axis_at else 1 for axis in range(len(shape))])
    return factor_of


def gaussian(rng, extent, width, bound, pieces=(), held_as=jnp.bfloat16):
    entries = jax.random.normal(rng, extent, jnp.float32) * width
    if len(pieces) > 0:
        entries = levels(rng, extent, pieces, -0.22, 0.18) * entries
    return jnp.clip(entries, min=-bound, max=bound).astype(held_as)


def setup_inputs(seed: int = 0) -> dict:
    streams_of = jax.random.split(jax.random.key(seed), 4)
    return {
        "velocity_u": gaussian(streams_of[0], (N, N, N), 1.0, 6.0, ((0, 4), (1, 32)), jnp.float32),
        "velocity_v": gaussian(streams_of[1], (N, N, N), 1.0, 6.0, ((0, 4), (1, 32)), jnp.float32),
        "scalar_theta": gaussian(streams_of[2], (N, N, N), 1.0, 6.0, ((0, 4), (1, 32)), jnp.float32),
    }


def transform_one(field):
    scale = 1.0 / (N * jnp.sqrt(jnp.float32(N)))
    index = ((jnp.arange(2 * KEEP) - KEEP) % N).astype(jnp.int32)
    spec = jnp.fft.rfft(field, axis=2)[:, :, :KEEP]
    spec = jnp.fft.fft(spec, axis=0)[index]
    spec = jnp.fft.fft(spec, axis=1)[:, index]
    spec = spec * scale
    result = jnp.concatenate([jnp.real(spec), jnp.imag(spec)], axis=-1).astype(jnp.float32)
    return result.at[KEEP, KEEP, 0].set(0.0)

def reference(velocity_u, velocity_v, scalar_theta):
    outputs = [transform_one(velocity_u * velocity_u), transform_one(velocity_v * velocity_v), transform_one(velocity_u * velocity_v), transform_one(velocity_u * scalar_theta)]
    return jnp.stack(outputs, axis=0)
```

```python
import functools

import jax
import jax.numpy as jnp
import numpy as np
from jax import lax
from jax.experimental import pallas as pl
from jax.experimental.pallas import tpu as pltpu
from jax.sharding import PartitionSpec as P

N = 512
KEEP = 160
MESH = pl.DeviceIdType.MESH
F32 = jnp.float32
BF16 = jnp.bfloat16
PITCH = 328
MIX_PITCH = 168
FACTORS = ((0, 0), (1, 1), (0, 1), (0, 2))


def split_table(table):
    high = table.astype(BF16)
    low = (table - high.astype(np.float64)).astype(BF16)
    return high, low


def waves(k, x):
    angle = (np.outer(k, x) % N) * (2.0 * np.pi / N)
    return np.cos(angle) / np.sqrt(N), np.sin(angle) / np.sqrt(N)


def depth_tables():
    cos, sin = waves(np.arange(KEEP), np.arange(N))
    real, imag = cos.T, -sin.T
    tables = np.zeros((2, N, 512))
    for parity in range(2):
        tables[parity, :, 0:128] = real[:, :128]
        tables[parity, :, 128:256] = imag[:, :128]
        at = 256 + 64 * parity
        tables[parity, :, at : at + 32] = real[:, 128:]
        tables[parity, :, at + 32 : at + 64] = imag[:, 128:]
        tables[parity, :, at + 128 : at + 160] = imag[:, 128:]
        tables[parity, :, at + 160 : at + 192] = -real[:, 128:]
    return split_table(tables)


def first_tables():
    tables = np.zeros((2, 640, 256))
    for half in range(2):
        x = np.arange(256) + 256 * half
        for side in range(2):
            cos, sin = waves(np.arange(KEEP) - KEEP * (1 - side), x)
            tables[half, side * 320 : side * 320 + 160] = cos
            tables[half, side * 320 + 160 : side * 320 + 320] = sin
    return split_table(tables)


def second_tables():
    tables = np.zeros((2, 2, 320, 256))
    y = np.arange(256)
    mixed = np.concatenate([2 * np.arange(128), 2 * np.arange(128) + 1])
    for parity in range(2):
        k = 2 * np.arange(KEEP) + parity - KEEP
        for order, places in enumerate((y, mixed)):
            cos, sin = waves(k, places)
            tables[parity, order] = np.concatenate([cos, sin], axis=0)
    return split_table(tables)


def halves(value):
    high = value.astype(BF16)
    return high, (value - high.astype(F32)).astype(BF16)


def dot(a, b):
    return jnp.dot(a, b, preferred_element_type=F32)


def exchange_kernel(
    u, v, t, zh, zl, xh, xl, ymain, ymix,
    fields, stack, zbuf, zout, xs, xr, xsm, xrm, dmain, dmix,
    in_sem, zs_sem, zr_sem, xs_sem, xr_sem, ds_sem, dr_sem, dl_sem,
):
    field, slab = lax.axis_index("field"), lax.axis_index("slab")
    hi, core = field // 2, field % 2
    lo, plane = slab // 16, slab % 16

    def peer_x(rel):
        half, side = (hi + rel // 2) % 2, (lo + rel % 2) % 2
        return half, side, {"field": half * 2 + core, "slab": side * 16 + plane}

    def peer_plane(step):
        other = (plane + step) % 16
        return other, {"field": field, "slab": lo * 16 + other}

    partner = {"field": hi * 2 + (1 - core), "slab": slab}
    loads = [
        pltpu.make_async_copy(ref.at[:, pl.ds(128 * part, 128)], fields.at[i, part], in_sem.at[i, part])
        for i, ref in enumerate((u, v, t))
        for part in range(4)
    ]
    for load in loads:
        load.start()

    barrier = pltpu.get_barrier_semaphore()
    pl.semaphore_signal(barrier, 1, device_id=partner, device_id_type=MESH)
    for rel in range(1, 4):
        pl.semaphore_signal(barrier, 1, device_id=peer_x(rel)[2], device_id_type=MESH)

    def greet(step, carry):
        pl.semaphore_signal(barrier, 1, device_id=peer_plane(step)[1], device_id_type=MESH)
        return carry

    lax.fori_loop(1, 16, greet, 0)
    pl.semaphore_wait(barrier, 19)
    for load in loads:
        load.wait()

    def z_copy(chunk):
        return pltpu.make_async_remote_copy(
            src_ref=zout.at[chunk % 6],
            dst_ref=zbuf.at[chunk, :, pl.ds(pl.multiple_of(core * 128, 128), 128), :],
            send_sem=zs_sem.at[chunk],
            recv_sem=zr_sem.at[chunk],
            device_id=partner,
            device_id_type=MESH,
        )

    def put_z(chunk, value):
        rows = pl.ds(pl.multiple_of(core * 128, 128), 128)
        for half in range(2):
            zbuf[chunk, half, rows, :] = value[half * 128 : half * 128 + 128]
            zout[chunk % 6, half] = value[256 + half * 128 : 384 + half * 128]
        z_copy(chunk).start()

    def depth_pair(pair):
        tail = None
        for parity in range(2):
            y = 2 * pair + parity
            for part in range(4):
                values = [fields[i, part, pl.ds(y, 128, stride=16), :] for i in range(3)]
                columns = slice(part * 128, part * 128 + 128)
                for product, (a, b) in enumerate(FACTORS):
                    high, low = halves(values[a] * values[b])
                    row = (product + core) % 2 * 256 + product // 2 * 128
                    stack[pl.ds(pl.multiple_of(row, 128), 128), columns] = high
                    stack[pl.ds(pl.multiple_of(row + 512, 128), 128), columns] = low
            both = dot(stack[...], zh[parity])
            value = both[:512] + both[512:] + dot(stack[:512], zl[parity])

            @pl.when(pair >= 2)
            def _():
                z_copy(3 * (pair - 2) + parity).wait_send()

            put_z(3 * pair + parity, value[:, :256])
            tail = value[:, 256:] if tail is None else tail + value[:, 256:]

        @pl.when(pair >= 2)
        def _():
            z_copy(3 * (pair - 2) + 2).wait_send()

        put_z(3 * pair + 2, tail)

    def first(chunk):
        z_copy(chunk).wait_recv()
        sides = []
        for half in range(2):
            high, low = halves(zbuf[chunk, half])
            mixed = dot(xh[hi], high) + dot(xh[hi], low) + dot(xl[hi], high)
            for side in range(2):
                sides.append((half, side, mixed[side * 320 : side * 320 + 160], mixed[side * 320 + 160 : side * 320 + 320]))
        return sides

    def main_rows(item):
        return pl.ds(pl.multiple_of(item * PITCH, 8), 320)

    def mix_rows(item):
        return pl.ds(pl.multiple_of(item * MIX_PITCH, 8), 160)

    def x_copy(rel, y):
        half, side, device = peer_x(rel)
        return pltpu.make_async_remote_copy(
            src_ref=xs.at[main_rows((half * 2 + side) * 16 + y), :],
            dst_ref=xr.at[main_rows((rel - 1) * 16 + y), :],
            send_sem=xs_sem.at[rel - 1, y],
            recv_sem=xr_sem.at[rel - 1, y],
            device_id=device,
            device_id_type=MESH,
        )

    def xm_copy(rel, pair):
        half, side, device = peer_x(rel)
        return pltpu.make_async_remote_copy(
            src_ref=xsm.at[mix_rows((half * 2 + side) * 8 + pair), :],
            dst_ref=xrm.at[mix_rows((rel - 1) * 8 + pair), :],
            send_sem=xs_sem.at[rel - 1, 16 + pair],
            recv_sem=xr_sem.at[rel - 1, 16 + pair],
            device_id=device,
            device_id_type=MESH,
        )

    def first_main(pair, parity):
        y = 2 * pair + parity
        for half, side, cos, sin in first(3 * pair + parity):
            rows = main_rows((half * 2 + side) * 16 + y)
            real = cos[:, :128] + sin[:, 128:]
            imag = cos[:, 128:] - sin[:, :128]
            xs[rows, :] = jnp.concatenate([real, imag], axis=0)
        for rel in (2, 1, 3):
            x_copy(rel, y).start()

    def first_mix(pair):
        for half, side, cos, sin in first(3 * pair + 2):
            xsm[mix_rows((half * 2 + side) * 8 + pair), :] = cos[:, :128] + sin[:, 128:]
        for rel in (2, 1, 3):
            xm_copy(rel, pair).start()

    def produce(pair, carry):
        depth_pair(pair)
        first_main(pair, 0)
        first_main(pair, 1)
        return carry

    lax.fori_loop(0, 8, produce, 0)

    def produce_mix(pair, carry):
        first_mix(pair)
        return carry

    lax.fori_loop(0, 8, produce_mix, 0)

    own = hi * 2 + lo

    def d_copy(group, block, step, device, other):
        near = (lo + block) % 2
        if group < 2:
            row = near * 256 + plane * 16 + group * 8
            src = dmain.at[block * 2 + group, pl.ds(other * 10, 10)]
            dst = ymain.at[:, pl.ds(pl.multiple_of(row, 8), 8), :]
        else:
            row = near * 128 + plane * 8
            src = dmix.at[block, pl.ds(other * 10, 10)]
            dst = ymix.at[:, pl.ds(pl.multiple_of(row, 8), 8), :]
        item = group * 2 + block
        if device is None:
            return pltpu.make_async_copy(src, dst, dl_sem.at[item])
        return pltpu.make_async_remote_copy(
            src_ref=src, dst_ref=dst, send_sem=ds_sem.at[item], recv_sem=dr_sem.at[item],
            device_id=device, device_id_type=MESH,
        )

    def send_group(group):
        for block in range(2):
            def go(step, carry):
                other, device = peer_plane(step)
                d_copy(group, block, step, device, other).start()
                return carry

            lax.fori_loop(1, 16, go, 0)
            d_copy(group, block, 0, None, plane).start()

    for group in range(2):
        for rel in range(1, 4):
            def arrive(y, carry):
                x_copy(rel, y).wait_recv()
                return carry

            lax.fori_loop(group * 8, group * 8 + 8, arrive, 0)

        def turn(k, carry):
            for part in range(2):
                base = group * 8 * PITCH + part * 160 + k
                columns = slice(part * 128, part * 128 + 128)

                def take(ref, item):
                    return ref[pl.ds(item * 16 * PITCH + base, 8, stride=PITCH), :]

                dmain[group, k, :, columns] = take(xs, own) + take(xr, 1)
                dmain[2 + group, k, :, columns] = take(xr, 0) + take(xr, 2)
            return carry

        lax.fori_loop(0, 160, turn, 0)
        send_group(group)

    for rel in range(1, 4):
        def arrive_mix(pair, carry):
            xm_copy(rel, pair).wait_recv()
            return carry

        lax.fori_loop(0, 8, arrive_mix, 0)

    def turn_mix(k, carry):
        def take(ref, item):
            return ref[pl.ds(item * 8 * MIX_PITCH + k, 8, stride=MIX_PITCH), :]

        dmix[0, k] = take(xsm, own) + take(xrm, 1)
        dmix[1, k] = take(xrm, 0) + take(xrm, 2)
        return carry

    lax.fori_loop(0, 160, turn_mix, 0)
    send_group(2)

    for chunk in range(18, 24):
        z_copy(chunk).wait_send()
    for rel in range(1, 4):
        def left(y, carry):
            x_copy(rel, y).wait_send()
            return carry

        lax.fori_loop(0, 16, left, 0)

        def left_mix(pair, carry):
            xm_copy(rel, pair).wait_send()
            return carry

        lax.fori_loop(0, 8, left_mix, 0)
    for group in range(3):
        for block in range(2):
            item = group * 2 + block
            whole = (dmain.at[block * 2 + group] if group < 2 else dmix.at[block]).at[pl.ds(0, 150)]
            pltpu.make_async_copy(whole, whole, ds_sem.at[item]).wait()
            pltpu.make_async_copy(whole, whole, dr_sem.at[item]).wait()
            d_copy(group, block, 0, None, plane).wait()


def exchange(u, v, t):
    zh, zl = depth_tables()
    xh, xl = first_tables()
    any_space = pl.BlockSpec(memory_space=pl.ANY)
    vmem = pl.BlockSpec(memory_space=pltpu.VMEM)
    return pl.pallas_call(
        exchange_kernel,
        out_shape=(
            jax.ShapeDtypeStruct((10, 512, 256), F32),
            jax.ShapeDtypeStruct((10, 256, 128), F32),
        ),
        in_specs=[any_space] * 3 + [vmem] * 4,
        out_specs=(any_space, any_space),
        scratch_shapes=[
            pltpu.VMEM((3, 4, 2048, 128), F32),
            pltpu.VMEM((1024, 512), BF16),
            pltpu.VMEM((24, 2, 256, 256), F32),
            pltpu.VMEM((6, 2, 128, 256), F32),
            pltpu.VMEM((4 * 16 * PITCH, 128), F32),
            pltpu.VMEM((3 * 16 * PITCH, 128), F32),
            pltpu.VMEM((4 * 8 * MIX_PITCH, 128), F32),
            pltpu.VMEM((3 * 8 * MIX_PITCH, 128), F32),
            pltpu.VMEM((4, 160, 8, 256), F32),
            pltpu.VMEM((2, 160, 8, 128), F32),
            pltpu.SemaphoreType.DMA((3, 4)),
            pltpu.SemaphoreType.DMA((24,)),
            pltpu.SemaphoreType.DMA((24,)),
            pltpu.SemaphoreType.DMA((3, 24)),
            pltpu.SemaphoreType.DMA((3, 24)),
            pltpu.SemaphoreType.DMA((6,)),
            pltpu.SemaphoreType.DMA((6,)),
            pltpu.SemaphoreType.DMA((6,)),
        ],
        compiler_params=pltpu.CompilerParams(
            collective_id=0, has_side_effects=True, vmem_limit_bytes=67043328
        ),
        name="exchange",
    )(u.reshape(2048, 512), v.reshape(2048, 512), t.reshape(2048, 512), zh, zl, xh, xl)


def second_kernel(main, mix, fh, fl, out, rows):
    slab = lax.axis_index("slab")
    row = slab * 10 + pl.program_id(0)
    low_y, high_y = main[0, :256, :], main[0, 256:, :]
    low_m, high_m = mix[0, :128, :], mix[0, 128:, :]
    for parity in range(2):
        if parity == 0:
            part, tail = low_y + high_y, low_m + high_m
        else:
            part, tail = low_y - high_y, low_m - high_m
        tail = jnp.concatenate([tail, pltpu.roll(tail, 64, 1)], axis=0)
        outs = []
        for order, value in ((0, part), (1, tail)):
            high, low = halves(value)
            a, b = fh[parity, order], fl[parity, order]
            outs.append(dot(a, high) + dot(a, low) + dot(b, high))
        wide, slim = outs
        cos, sin = wide[:160], wide[160:]
        real = cos[:, :128] + sin[:, 128:]
        imag = cos[:, 128:] - sin[:, :128]
        cos, sin = slim[:160], slim[160:]
        tail_real = cos + pltpu.roll(sin, 96, 1)
        tail_imag = cos - pltpu.roll(sin, 32, 1)
        result = jnp.concatenate(
            [real, tail_real[:, :32], imag, tail_imag[:, 32:64], jnp.zeros((160, 64), F32)], axis=1
        )
        if parity == 0:
            at_row = lax.broadcasted_iota(jnp.int32, (160, 384), 0)
            at_col = lax.broadcasted_iota(jnp.int32, (160, 384), 1)
            zero = (at_row == 80) & (at_col == 0) & (row == KEEP)
            result = jnp.where(zero, 0.0, result)
        for part in range(3):
            rows[part, pl.ds(parity, 160, stride=2), :] = result[:, part * 128 : part * 128 + 128]
    out[0, 0, :, :128] = rows[0]
    out[0, 0, :, 128:256] = rows[1]
    out[0, 0, :, 256:] = rows[2, :, :64]


def second(main, mix):
    fh, fl = second_tables()
    whole = pl.BlockSpec((2, 2, 320, 256), lambda i: (0, 0, 0, 0))
    return pl.pallas_call(
        second_kernel,
        grid=(10,),
        out_shape=jax.ShapeDtypeStruct((1, 10, 320, 320), F32),
        in_specs=[
            pl.BlockSpec((1, 512, 256), lambda i: (i, 0, 0)),
            pl.BlockSpec((1, 256, 128), lambda i: (i, 0, 0)),
            whole,
            whole,
        ],
        out_specs=pl.BlockSpec((1, 1, 320, 320), lambda i: (0, i, 0, 0)),
        scratch_shapes=[pltpu.VMEM((3, 320, 128), F32)],
        compiler_params=pltpu.CompilerParams(dimension_semantics=("arbitrary",)),
        name="second",
    )(main, mix, fh, fl)


def shards(velocity_u, velocity_v, scalar_theta):
    main, mix = exchange(velocity_u, velocity_v, scalar_theta)
    return second(main, mix)


def solution(mesh):
    spec = P("field", "slab", None)
    return jax.shard_map(
        shards,
        mesh=mesh,
        in_specs=(spec, spec, spec),
        out_specs=P("field", "slab", None, None),
        check_vma=False,
    )
```

```python
import functools

import jax
import jax.numpy as jnp
import numpy as np
from jax import lax
from jax.experimental import pallas as pl
from jax.experimental.pallas import tpu as pltpu
from jax.sharding import PartitionSpec as P

N = 512
KEEP = 160
MESH = pl.DeviceIdType.MESH
F32 = jnp.float32
BF16 = jnp.bfloat16
GROUPS = (4, 3, 1, 1, 1)
STARTS = (0, 4, 7, 8, 9)
STEPS = (
    ((0, 1), (1, 0), (0, 3), (3, 0), (1, 1), (3, 3), (1, 3), (3, 1))
    + ((2, 1), (2, 3), (0, 2), (2, 0), (2, 2))
    + ((1, 2), (3, 2))
)
PITCH = 328
MIX_PITCH = 168
FACTORS = ((0, 0), (1, 1), (0, 1), (0, 2))


def split_table(table):
    high = table.astype(BF16)
    low = (table - high.astype(np.float64)).astype(BF16)
    return high, low


def waves(k, x):
    angle = (np.outer(k, x) % N) * (2.0 * np.pi / N)
    return np.cos(angle) / np.sqrt(N), np.sin(angle) / np.sqrt(N)


def depth_tables():
    cos, sin = waves(np.arange(KEEP), np.arange(N))
    real, imag = cos.T, -sin.T
    tables = np.zeros((3, N, 256))
    tables[0, :, :128] = real[:, :128]
    tables[0, :, 128:] = imag[:, :128]
    for parity in range(2):
        at = 64 * parity
        tables[1 + parity, :, at : at + 32] = real[:, 128:]
        tables[1 + parity, :, at + 32 : at + 64] = imag[:, 128:]
        tables[1 + parity, :, at + 128 : at + 160] = imag[:, 128:]
        tables[1 + parity, :, at + 160 : at + 192] = -real[:, 128:]
    return split_table(tables)


def first_tables():
    order = (10 * np.arange(16)[None, :] + np.arange(11)[:, None]).reshape(-1)
    tables = np.zeros((2, 352, 256))
    for half in range(2):
        tables[half] = np.concatenate(waves(order, np.arange(256) + 256 * half), axis=0)
    return split_table(tables)


def second_tables():
    tables = np.zeros((2, 2, 320, 256))
    y = np.arange(256)
    mixed = np.concatenate([2 * np.arange(128), 2 * np.arange(128) + 1])
    for parity in range(2):
        k = 2 * np.arange(KEEP) + parity - KEEP
        for order, places in enumerate((y, mixed)):
            cos, sin = waves(k, places)
            tables[parity, order] = np.concatenate([cos, sin], axis=0)
    return split_table(tables)


def halves(value):
    high = value.astype(BF16)
    return high, (value - high.astype(F32)).astype(BF16)


def dot(a, b):
    return jnp.dot(a, b, preferred_element_type=F32)


def second_rows(lift, fh, fl, rows, row):
    real_of = [lift(40 * a, 16) for a in range(2)]
    imag_of = [lift(40 * a + 16, 16) for a in range(2)]
    tail_of = [lift(40 * a + 32, 8) for a in range(2)]
    for parity in range(2):

        def fold(pair):
            return pair[0] + pair[1] if parity == 0 else pair[0] - pair[1]

        part = jnp.concatenate([fold(real_of), fold(imag_of)], axis=1)
        tail = fold(tail_of)
        tail = jnp.concatenate([tail, pltpu.roll(tail, 64, 1)], axis=0)
        outs = []
        for order, value in ((0, part), (1, tail)):
            high, low = halves(value)
            a, b = fh[parity, order], fl[parity, order]
            outs.append(dot(a, high) + dot(a, low) + dot(b, high))
        wide, slim = outs
        cos, sin = wide[:160], wide[160:]
        real = cos[:, :128] + sin[:, 128:]
        imag = cos[:, 128:] - sin[:, :128]
        cos, sin = slim[:160], slim[160:]
        tail_real = cos + pltpu.roll(sin, 96, 1)
        tail_imag = cos - pltpu.roll(sin, 32, 1)
        result = jnp.concatenate(
            [real, tail_real[:, :32], imag, tail_imag[:, 32:64], jnp.zeros((160, 64), F32)], axis=1
        )
        if parity == 0:
            at_row = lax.broadcasted_iota(jnp.int32, (160, 384), 0)
            at_col = lax.broadcasted_iota(jnp.int32, (160, 384), 1)
            zero = (at_row == 80) & (at_col == 0) & (row == KEEP)
            result = jnp.where(zero, 0.0, result)
        for place in range(3):
            rows[place, pl.ds(parity, 160, stride=2), :] = result[:, place * 128 : place * 128 + 128]


def exchange_kernel(
    u, v, t, zh, zl, xh, xl, fh, fl, yall, parts,
    fields, zth, ztl, xth, xtl, fth, ftl, stack, held, zbuf, zout, xs, xr, xsm, xrm, dall, rows,
    in_sem, tab_sem, zs_sem, zr_sem, xs_sem, xr_sem, ds_sem, dr_sem, dl_sem, y_sem, p_sem,
):
    field, slab = lax.axis_index("field"), lax.axis_index("slab")
    hi, core = field // 2, field % 2
    lo, plane = slab // 16, slab % 16
    own = hi * 2 + lo

    def peer_x(rel):
        half, side = (hi + rel // 2) % 2, (lo + rel % 2) % 2
        return half, side, {"field": half * 2 + core, "slab": side * 16 + plane}

    def peer_plane(step):
        other = (plane // 4 + step[0]) % 4 * 4 + (plane + step[1]) % 4
        return other, {"field": field, "slab": lo * 16 + other}

    partner = {"field": hi * 2 + (1 - core), "slab": slab}

    def loads(octet):
        return [
            pltpu.make_async_copy(
                ref.at[:, pl.ds(8 * octet, 8), pl.ds(128 * part, 128)],
                fields.at[i, part, octet],
                in_sem.at[octet, i, part],
            )
            for part in range(4)
            for i, ref in enumerate((u, v, t))
        ]

    tables = [
        pltpu.make_async_copy(src, dst, tab_sem.at[i])
        for i, (src, dst) in enumerate(
            ((zh, zth), (zl, ztl), (xh.at[hi], xth), (xl.at[hi], xtl), (fh, fth), (fl, ftl))
        )
    ]
    tables[0].start()
    for load in loads(0):
        load.start()
    for table in tables[1:4]:
        table.start()
    for load in loads(1):
        load.start()
    for table in tables[4:]:
        table.start()

    barrier = pltpu.get_barrier_semaphore()
    pl.semaphore_signal(barrier, 1, device_id=partner, device_id_type=MESH)
    for rel in range(1, 4):
        pl.semaphore_signal(barrier, 1, device_id=peer_x(rel)[2], device_id_type=MESH)

    for step in STEPS:
        pl.semaphore_signal(barrier, 1, device_id=peer_plane(step)[1], device_id_type=MESH)
    pl.semaphore_wait(barrier, 19)

    def z_slot(chunk):
        return jnp.where(chunk < 16, chunk % 4, 4 + chunk % 2)

    def z_copy(chunk):
        return pltpu.make_async_remote_copy(
            src_ref=zout.at[z_slot(chunk)],
            dst_ref=zbuf.at[chunk, :, pl.ds(pl.multiple_of(core * 128, 128), 128), :],
            send_sem=zs_sem.at[chunk],
            recv_sem=zr_sem.at[chunk],
            device_id=partner,
            device_id_type=MESH,
        )

    def put_z(chunk, value):
        rows = pl.ds(pl.multiple_of(core * 128, 128), 128)
        for half in range(2):
            zbuf[chunk, half, rows, :] = value[half * 128 : half * 128 + 128]
            zout[z_slot(chunk), half] = value[256 + half * 128 : 384 + half * 128]
        z_copy(chunk).start()

    flat = fields.reshape(3, 4, 2048, 128)

    def depth_by(table):
        both = dot(stack[...], zth[table])
        return both[:512] + both[512:] + dot(stack[:512], ztl[table])

    def depth_main(y):
        for part in range(4):
            rows = pl.ds((y // 8) * 1024 + y % 8, 128, stride=8)
            values = [flat[i, part, rows, :] for i in range(3)]
            columns = slice(part * 128, part * 128 + 128)
            for product, (a, b) in enumerate(FACTORS):
                high, low = halves(values[a] * values[b])
                row = (product + core) % 2 * 256 + product // 2 * 128
                stack[pl.ds(pl.multiple_of(row, 128), 128), columns] = high
                stack[pl.ds(pl.multiple_of(row + 512, 128), 128), columns] = low

        @pl.when(y >= 4)
        def _():
            z_copy(y - 4).wait_send()

        put_z(y, depth_by(0))

    def depth_tail(y):
        tail = depth_by(1 + y % 2)

        @pl.when(y % 2 == 0)
        def _():
            held[...] = tail

        @pl.when(y % 2 == 1)
        def _():
            @pl.when(y >= 4)
            def _():
                z_copy(16 + y // 2 - 2).wait_send()

            put_z(16 + y // 2, held[...] + tail)

    def first(chunk):
        z_copy(chunk).wait_recv()
        pairs = []
        for half in range(2):
            high, low = halves(zbuf[chunk, half])
            mixed = dot(xth[...], high) + dot(xth[...], low) + dot(xtl[...], high)
            pairs.append((half, mixed[:176], mixed[176:]))
        return pairs

    def rows_at(side, i):
        return 16 * i if side == 1 else 16 * (10 - i)

    def x_copy(rel, y, group):
        half, side, device = peer_x(rel)
        at, count = 32 * STARTS[group], 32 * GROUPS[group]

        def rows(item):
            return pl.ds(pl.multiple_of(item * PITCH + at, 8), count)

        return pltpu.make_async_remote_copy(
            src_ref=xs.at[rows((half * 2 + side) * 16 + y), :],
            dst_ref=xr.at[rows((rel - 1) * 16 + y), :],
            send_sem=xs_sem.at[0, rel - 1, group],
            recv_sem=xr_sem.at[0, rel - 1, group],
            device_id=device,
            device_id_type=MESH,
        )

    def xm_copy(rel, pair, group):
        half, side, device = peer_x(rel)
        at, count = 16 * STARTS[group], 16 * GROUPS[group]

        def rows(item):
            return pl.ds(pl.multiple_of(item * MIX_PITCH + at, 8), count)

        return pltpu.make_async_remote_copy(
            src_ref=xsm.at[rows((half * 2 + side) * 8 + pair), :],
            dst_ref=xrm.at[rows((rel - 1) * 8 + pair), :],
            send_sem=xs_sem.at[1, rel - 1, group],
            recv_sem=xr_sem.at[1, rel - 1, group],
            device_id=device,
            device_id_type=MESH,
        )

    def first_main(y):
        for half, cos, sin in first(y):
            for side in range(2):
                base = ((half * 2 + side) * 16 + y) * PITCH
                sign = 1.0 if side == 1 else -1.0
                real = cos[:, :128] + sign * sin[:, 128:]
                imag = cos[:, 128:] - sign * sin[:, :128]
                for i0, count in zip(STARTS, GROUPS):
                    at = base + 32 * i0
                    for i in range(count):
                        rows = slice(rows_at(side, i0 + i), rows_at(side, i0 + i) + 16)
                        xs[pl.ds(pl.multiple_of(at + 16 * i, 8), 16), :] = real[rows]
                        xs[pl.ds(pl.multiple_of(at + 16 * (count + i), 8), 16), :] = imag[rows]
        for rel in (2, 1, 3):
            x_copy(rel, y, 0).start()

    def first_mix(pair):
        for half, cos, sin in first(16 + pair):
            for side in range(2):
                at = ((half * 2 + side) * 8 + pair) * MIX_PITCH
                sign = 1.0 if side == 1 else -1.0
                value = cos[:, :128] + sign * sin[:, 128:]
                for i in range(10):
                    rows = slice(rows_at(side, i), rows_at(side, i) + 16)
                    xsm[pl.ds(pl.multiple_of(at + 16 * i, 8), 16), :] = value[rows]
        for rel in (2, 1, 3):
            xm_copy(rel, pair, 0).start()

    tables[0].wait()
    for load in loads(0):
        load.wait()
    for table in tables[1:4]:
        table.wait()

    def produce(step, carry):
        @pl.when(step == 8)
        def _():
            for load in loads(1):
                load.wait()

        @pl.when(step < 16)
        def _():
            depth_main(step)

        @pl.when(step != 1)
        def _():
            first_main(jnp.maximum(step - 1, 0))

        @pl.when(step < 16)
        def _():
            depth_tail(step)

        return carry

    lax.fori_loop(0, 17, produce, 0)

    def produce_mix(pair, carry):
        first_mix(pair)
        return carry

    lax.fori_loop(0, 8, produce_mix, 0)

    def send_x(group):
        def go(y, carry):
            for rel in (2, 1, 3):
                x_copy(rel, y, group).start()
            return carry

        lax.fori_loop(0, 16, go, 0)

        def go_mix(pair, carry):
            for rel in (2, 1, 3):
                xm_copy(rel, pair, group).start()
            return carry

        lax.fori_loop(0, 8, go_mix, 0)

    def d_copy(group, device, other):
        span = pl.ds(STARTS[group], GROUPS[group])
        src = dall.at[other, span]
        dst = yall.at[span, pl.ds(pl.multiple_of(plane * 80, 80), 80), :]
        if device is None:
            return pltpu.make_async_copy(src, dst, dl_sem.at[group])
        return pltpu.make_async_remote_copy(
            src_ref=src,
            dst_ref=dst,
            send_sem=ds_sem.at[group],
            recv_sem=dr_sem.at[group],
            device_id=device,
            device_id_type=MESH,
        )

    def turn(group):
        i0, count = STARTS[group], GROUPS[group]
        near, far = lo * 40, (1 - lo) * 40

        def go(r, carry):
            i, place = i0 + r // 16, r % 16
            other = lo * place + (1 - lo) * (15 - place)

            def put(offset, near_value, far_value):
                dall[other, i, pl.ds(pl.multiple_of(near + offset, 8), 8), :] = near_value
                dall[other, i, pl.ds(pl.multiple_of(far + offset, 8), 8), :] = far_value

            for part in range(2):
                for octet in range(2):
                    base = octet * 8 * PITCH + 32 * i0 + part * 16 * count + r

                    def take(ref, item):
                        return ref[pl.ds(item * 16 * PITCH + base, 8, stride=PITCH), :]

                    put(part * 16 + octet * 8, take(xs, own) + take(xr, 1), take(xr, 0) + take(xr, 2))

            def take_mix(ref, item):
                return ref[pl.ds(item * 8 * MIX_PITCH + 16 * i0 + r, 8, stride=MIX_PITCH), :]

            put(32, take_mix(xsm, own) + take_mix(xrm, 1), take_mix(xrm, 0) + take_mix(xrm, 2))
            return carry

        lax.fori_loop(0, 16 * count, go, 0)

    def x_wait(group, sem):
        main = xr.at[pl.ds(0, 512 * GROUPS[group]), :]
        mix = xrm.at[pl.ds(0, 128 * GROUPS[group]), :]
        for rel in range(3):
            pltpu.make_async_copy(main, main, sem.at[0, rel, group]).wait()
            pltpu.make_async_copy(mix, mix, sem.at[1, rel, group]).wait()

    lines = fields.reshape(24576, 128)

    def y_load(i):
        return pltpu.make_async_copy(
            yall.at[i], lines.at[pl.ds(pl.multiple_of(i * 1280, 1280), 1280), :], y_sem.at[i]
        )

    def part_copy(i):
        return pltpu.make_async_copy(rows.at[i % 2], parts.at[i], p_sem.at[i])

    def second(group):
        whole = dall.at[pl.ds(0, 15), pl.ds(0, GROUPS[group])]
        pltpu.make_async_copy(whole, whole, dr_sem.at[group]).wait()
        d_copy(group, None, plane).wait()
        first_i, last_i = STARTS[group], STARTS[group] + GROUPS[group]
        for i in range(first_i, last_i):
            y_load(i).start()

        def go(i, carry):
            y_load(i).wait()

            @pl.when(i >= 2)
            def _():
                part_copy(i - 2).wait()

            def lift(offset, count):
                return jnp.concatenate(
                    [
                        lines[pl.ds(pl.multiple_of(i * 1280 + 80 * j + offset, 8), count), :]
                        for j in range(16)
                    ],
                    axis=0,
                )

            second_rows(lift, fth, ftl, rows.at[i % 2], slab * 10 + i)
            part_copy(i).start()
            return carry

        lax.fori_loop(first_i, last_i, go, 0)

    for group in range(len(GROUPS)):
        if group + 1 < len(GROUPS):
            send_x(group + 1)
        x_wait(group, xr_sem)
        turn(group)

        for step in STEPS:
            other, device = peer_plane(step)
            d_copy(group, device, other).start()
        d_copy(group, None, plane).start()
        if group == 0:
            for table in tables[4:]:
                table.wait()
        else:
            second(group - 1)

    def z_left(chunk, carry):
        z_copy(chunk).wait_send()
        return carry

    lax.fori_loop(12, 16, z_left, 0)
    lax.fori_loop(22, 24, z_left, 0)
    for group in range(len(GROUPS)):
        x_wait(group, xs_sem)
    second(len(GROUPS) - 1)
    for group in range(len(GROUPS)):
        whole = dall.at[pl.ds(0, 15), pl.ds(0, GROUPS[group])]
        pltpu.make_async_copy(whole, whole, ds_sem.at[group]).wait()
    part_copy(8).wait()
    part_copy(9).wait()


def exchange(u, v, t):
    zh, zl = depth_tables()
    xh, xl = first_tables()
    fh, fl = second_tables()
    groups = len(GROUPS)
    any_space = pl.BlockSpec(memory_space=pl.ANY)
    return pl.pallas_call(
        exchange_kernel,
        out_shape=(
            jax.ShapeDtypeStruct((10, 1280, 128), F32),
            jax.ShapeDtypeStruct((10, 3, 320, 128), F32),
        ),
        in_specs=[any_space] * 9,
        out_specs=(any_space, any_space),
        scratch_shapes=[
            pltpu.VMEM((3, 4, 2, 128, 8, 128), F32),
            pltpu.VMEM((3, 512, 256), BF16),
            pltpu.VMEM((3, 512, 256), BF16),
            pltpu.VMEM((352, 256), BF16),
            pltpu.VMEM((352, 256), BF16),
            pltpu.VMEM((2, 2, 320, 256), BF16),
            pltpu.VMEM((2, 2, 320, 256), BF16),
            pltpu.VMEM((1024, 512), BF16),
            pltpu.VMEM((512, 256), F32),
            pltpu.VMEM((24, 2, 256, 256), F32),
            pltpu.VMEM((6, 2, 128, 256), F32),
            pltpu.VMEM((4 * 16 * PITCH, 128), F32),
            pltpu.VMEM((3 * 16 * PITCH, 128), F32),
            pltpu.VMEM((4 * 8 * MIX_PITCH, 128), F32),
            pltpu.VMEM((3 * 8 * MIX_PITCH, 128), F32),
            pltpu.VMEM((16, 10, 80, 128), F32),
            pltpu.VMEM((2, 3, 320, 128), F32),
            pltpu.SemaphoreType.DMA((2, 3, 4)),
            pltpu.SemaphoreType.DMA((6,)),
            pltpu.SemaphoreType.DMA((24,)),
            pltpu.SemaphoreType.DMA((24,)),
            pltpu.SemaphoreType.DMA((2, 3, groups)),
            pltpu.SemaphoreType.DMA((2, 3, groups)),
            pltpu.SemaphoreType.DMA((groups,)),
            pltpu.SemaphoreType.DMA((groups,)),
            pltpu.SemaphoreType.DMA((groups,)),
            pltpu.SemaphoreType.DMA((10,)),
            pltpu.SemaphoreType.DMA((10,)),
        ],
        compiler_params=pltpu.CompilerParams(
            collective_id=0, has_side_effects=True, vmem_limit_bytes=67043328
        ),
        name="exchange",
    )(u, v, t, zh, zl, xh, xl, fh, fl)


def lay_out_kernel(parts, out):
    for i in range(2):
        out[0, i, :, :128] = parts[i, 0]
        out[0, i, :, 128:256] = parts[i, 1]
        out[0, i, :, 256:] = parts[i, 2, :, :64]


def lay_out(parts):
    return pl.pallas_call(
        lay_out_kernel,
        grid=(5,),
        out_shape=jax.ShapeDtypeStruct((1, 10, 320, 320), F32),
        in_specs=[pl.BlockSpec((2, 3, 320, 128), lambda i: (i, 0, 0, 0))],
        out_specs=pl.BlockSpec((1, 2, 320, 320), lambda i: (0, i, 0, 0)),
        compiler_params=pltpu.CompilerParams(dimension_semantics=("arbitrary",)),
        name="lay_out",
    )(parts)


def shards(velocity_u, velocity_v, scalar_theta):
    return lay_out(exchange(velocity_u, velocity_v, scalar_theta)[1])


def solution(mesh):
    spec = P("field", "slab", None)
    return jax.shard_map(
        shards,
        mesh=mesh,
        in_specs=(spec, spec, spec),
        out_specs=P("field", "slab", None, None),
        check_vma=False,
    )
```

```python
import functools

import jax
import jax.numpy as jnp
import numpy as np
from jax import lax
from jax.experimental import pallas as pl
from jax.experimental.pallas import tpu as pltpu
from jax.sharding import PartitionSpec as P

N = 512
KEEP = 160
MESH = pl.DeviceIdType.MESH
F32 = jnp.float32
BF16 = jnp.bfloat16
GROUPS = (3, 3, 2, 1, 1)
STARTS = (0, 3, 6, 8, 9)
LAST = 4
PHASES = ((0, 0, 2, True), (1, 0, 2, True), (2, 0, 2, True), (3, 0, 2, True), (4, 0, 1, False), (4, 1, 2, False), (4, 2, 2, True))
STEPS = (
    ((0, 1), (1, 0), (0, 3), (3, 0), (1, 1), (3, 3), (1, 3), (3, 1))
    + ((2, 1), (2, 3), (0, 2), (2, 0), (2, 2))
    + ((1, 2), (3, 2))
)
EARLY = 8
PITCH = 328
MIX_PITCH = 168
FACTORS = ((0, 0), (1, 1), (0, 1), (0, 2))


def split_table(table):
    high = table.astype(BF16)
    low = (table - high.astype(np.float64)).astype(BF16)
    return high, low


def waves(k, x):
    angle = (np.outer(k, x) % N) * (2.0 * np.pi / N)
    return np.cos(angle) / np.sqrt(N), np.sin(angle) / np.sqrt(N)


def depth_tables():
    cos, sin = waves(np.arange(KEEP), np.arange(N))
    real, imag = cos.T, -sin.T
    tables = np.zeros((3, N, 256))
    tables[0, :, :128] = real[:, :128]
    tables[0, :, 128:] = imag[:, :128]
    for parity in range(2):
        at = 64 * parity
        tables[1 + parity, :, at : at + 32] = real[:, 128:]
        tables[1 + parity, :, at + 32 : at + 64] = imag[:, 128:]
        tables[1 + parity, :, at + 128 : at + 160] = imag[:, 128:]
        tables[1 + parity, :, at + 160 : at + 192] = -real[:, 128:]
    return split_table(tables)


def first_tables():
    order = (10 * np.arange(16)[None, :] + np.arange(11)[:, None]).reshape(-1)
    tables = np.zeros((2, 352, 256))
    for half in range(2):
        tables[half] = np.concatenate(waves(order, np.arange(256) + 256 * half), axis=0)
    return split_table(tables)


def second_tables():
    tables = np.zeros((2, 2, 320, 256))
    y = np.arange(256)
    mixed = np.concatenate([2 * np.arange(128), 2 * np.arange(128) + 1])
    for parity in range(2):
        k = 2 * np.arange(KEEP) + parity - KEEP
        for order, places in enumerate((y, mixed)):
            cos, sin = waves(k, places)
            tables[parity, order] = np.concatenate([cos, sin], axis=0)
    return split_table(tables)


def halves(value):
    high = value.astype(BF16)
    return high, (value - high.astype(F32)).astype(BF16)


def dot(a, b):
    return jnp.dot(a, b, preferred_element_type=F32)


def second_rows(lift, fh, fl, rows, row):
    real_of = [lift((16 * a, 32 + 16 * a)) for a in range(2)]
    imag_of = [lift((16 * a + 8, 40 + 16 * a)) for a in range(2)]
    tail_of = [lift((64 + 8 * a,)) for a in range(2)]
    for parity in range(2):

        def fold(pair):
            return pair[0] + pair[1] if parity == 0 else pair[0] - pair[1]

        part = jnp.concatenate([fold(real_of), fold(imag_of)], axis=1)
        tail = fold(tail_of)
        tail = jnp.concatenate([tail, pltpu.roll(tail, 64, 1)], axis=0)
        outs = []
        for order, value in ((0, part), (1, tail)):
            high, low = halves(value)
            a, b = fh[parity, order], fl[parity, order]
            outs.append(dot(a, high) + dot(a, low) + dot(b, high))
        wide, slim = outs
        cos, sin = wide[:160], wide[160:]
        real = cos[:, :128] + sin[:, 128:]
        imag = cos[:, 128:] - sin[:, :128]
        cos, sin = slim[:160], slim[160:]
        tail_real = cos + pltpu.roll(sin, 96, 1)
        tail_imag = cos - pltpu.roll(sin, 32, 1)
        result = jnp.concatenate(
            [real, tail_real[:, :32], imag, tail_imag[:, 32:64], jnp.zeros((160, 64), F32)], axis=1
        )
        if parity == 0:
            at_row = lax.broadcasted_iota(jnp.int32, (160, 384), 0)
            at_col = lax.broadcasted_iota(jnp.int32, (160, 384), 1)
            zero = (at_row == 80) & (at_col == 0) & (row == KEEP)
            result = jnp.where(zero, 0.0, result)
        for place in range(3):
            rows[place, pl.ds(parity, 160, stride=2), :] = result[:, place * 128 : place * 128 + 128]


def exchange_kernel(
    u, v, t, zh, zl, xh, xl, fh, fl, yall, parts,
    fields, zth, ztl, xth, xtl, fth, ftl, stack, held, zbuf, zout, xs, xr, xsm, xrm, dall, ylast, rows,
    in_sem, tab_sem, zs_sem, zr_sem, xs_sem, xr_sem, ds_sem, dr_sem, dl_sem, y_sem, p_sem,
):
    field, slab = lax.axis_index("field"), lax.axis_index("slab")
    hi, core = field // 2, field % 2
    lo, plane = slab // 16, slab % 16
    own = hi * 2 + lo

    def peer_x(rel):
        half, side = (hi + rel // 2) % 2, (lo + rel % 2) % 2
        return half, side, {"field": half * 2 + core, "slab": side * 16 + plane}

    def peer_plane(step):
        other = (plane // 4 + step[0]) % 4 * 4 + (plane + step[1]) % 4
        return other, {"field": field, "slab": lo * 16 + other}

    partner = {"field": hi * 2 + (1 - core), "slab": slab}

    def loads(octet):
        return [
            pltpu.make_async_copy(
                ref.at[:, pl.ds(8 * octet, 8), pl.ds(128 * part, 128)],
                fields.at[i, part, octet],
                in_sem.at[octet, i, part],
            )
            for part in range(4)
            for i, ref in enumerate((u, v, t))
        ]

    tables = [
        pltpu.make_async_copy(src, dst, tab_sem.at[i])
        for i, (src, dst) in enumerate(
            (
                (zh.at[0], zth.at[0]), (zl.at[0], ztl.at[0]), (xh.at[hi], xth), (xl.at[hi], xtl),
                (zh.at[pl.ds(1, 2)], zth.at[pl.ds(1, 2)]), (zl.at[pl.ds(1, 2)], ztl.at[pl.ds(1, 2)]),
                (fh, fth), (fl, ftl),
            )
        )
    ]
    tables[0].start()
    tables[1].start()
    for load in loads(0):
        load.start()
    for table in tables[2:4]:
        table.start()

    barrier = pltpu.get_barrier_semaphore()
    pl.semaphore_signal(barrier, 1, device_id=partner, device_id_type=MESH)
    for rel in range(1, 4):
        pl.semaphore_signal(barrier, 1, device_id=peer_x(rel)[2], device_id_type=MESH)

    for step in STEPS:
        pl.semaphore_signal(barrier, 1, device_id=peer_plane(step)[1], device_id_type=MESH)
    pl.semaphore_wait(barrier, 19)

    def z_slot(chunk):
        return jnp.where(chunk < 16, chunk % 4, 4 + chunk % 2)

    def z_copy(chunk):
        return pltpu.make_async_remote_copy(
            src_ref=zout.at[z_slot(chunk)],
            dst_ref=zbuf.at[chunk, :, pl.ds(pl.multiple_of(core * 128, 128), 128), :],
            send_sem=zs_sem.at[chunk],
            recv_sem=zr_sem.at[chunk],
            device_id=partner,
            device_id_type=MESH,
        )

    def put_z(chunk, value):
        rows = pl.ds(pl.multiple_of(core * 128, 128), 128)
        for half in range(2):
            zbuf[chunk, half, rows, :] = value[half * 128 : half * 128 + 128]
            zout[z_slot(chunk), half] = value[256 + half * 128 : 384 + half * 128]
        z_copy(chunk).start()

    flat = fields.reshape(3, 4, 2048, 128)

    def depth_by(table):
        both = dot(stack[...], zth[table])
        return both[:512] + both[512:] + dot(stack[:512], ztl[table])

    def depth_main(y):
        for part in range(4):
            rows = pl.ds((y // 8) * 1024 + y % 8, 128, stride=8)
            values = [flat[i, part, rows, :] for i in range(3)]
            columns = slice(part * 128, part * 128 + 128)
            for product, (a, b) in enumerate(FACTORS):
                high, low = halves(values[a] * values[b])
                row = (product + core) % 2 * 256 + product // 2 * 128
                stack[pl.ds(pl.multiple_of(row, 128), 128), columns] = high
                stack[pl.ds(pl.multiple_of(row + 512, 128), 128), columns] = low

        @pl.when(y >= 4)
        def _():
            z_copy(y - 4).wait_send()

        put_z(y, depth_by(0))

    def depth_tail(y):
        tail = depth_by(1 + y % 2)

        @pl.when(y % 2 == 0)
        def _():
            held[...] = tail

        @pl.when(y % 2 == 1)
        def _():
            @pl.when(y >= 4)
            def _():
                z_copy(16 + y // 2 - 2).wait_send()

            put_z(16 + y // 2, held[...] + tail)

    def first(chunk):
        z_copy(chunk).wait_recv()
        pairs = []
        for half in range(2):
            high, low = halves(zbuf[chunk, half])
            mixed = dot(xth[...], high) + dot(xth[...], low) + dot(xtl[...], high)
            pairs.append((half, mixed[:176], mixed[176:]))
        return pairs

    def rows_at(side, i):
        return 16 * i if side == 1 else 16 * (10 - i)

    def x_copy(rel, y, phase):
        half, side, device = peer_x(rel)
        group = PHASES[phase][0]
        at, count = 32 * STARTS[group], 32 * GROUPS[group]

        def rows(item):
            return pl.ds(pl.multiple_of(item * PITCH + at, 8), count)

        return pltpu.make_async_remote_copy(
            src_ref=xs.at[rows((half * 2 + side) * 16 + y), :],
            dst_ref=xr.at[rows((rel - 1) * 16 + y), :],
            send_sem=xs_sem.at[0, rel - 1, phase],
            recv_sem=xr_sem.at[0, rel - 1, phase],
            device_id=device,
            device_id_type=MESH,
        )

    def xm_copy(rel, pair, phase):
        half, side, device = peer_x(rel)
        group = PHASES[phase][0]
        at, count = 16 * STARTS[group], 16 * GROUPS[group]

        def rows(item):
            return pl.ds(pl.multiple_of(item * MIX_PITCH + at, 8), count)

        return pltpu.make_async_remote_copy(
            src_ref=xsm.at[rows((half * 2 + side) * 8 + pair), :],
            dst_ref=xrm.at[rows((rel - 1) * 8 + pair), :],
            send_sem=xs_sem.at[1, rel - 1, phase],
            recv_sem=xr_sem.at[1, rel - 1, phase],
            device_id=device,
            device_id_type=MESH,
        )

    def first_main(y):
        for half, cos, sin in first(y):
            for side in range(2):
                base = ((half * 2 + side) * 16 + y) * PITCH
                sign = 1.0 if side == 1 else -1.0
                real = cos[:, :128] + sign * sin[:, 128:]
                imag = cos[:, 128:] - sign * sin[:, :128]
                for i0, count in zip(STARTS, GROUPS):
                    at = base + 32 * i0
                    for i in range(count):
                        rows = slice(rows_at(side, i0 + i), rows_at(side, i0 + i) + 16)
                        xs[pl.ds(pl.multiple_of(at + 16 * i, 8), 16), :] = real[rows]
                        xs[pl.ds(pl.multiple_of(at + 16 * (count + i), 8), 16), :] = imag[rows]
        for rel in (2, 1, 3):
            x_copy(rel, y, 0).start()

        @pl.when(y < EARLY)
        def _():
            for rel in (2, 1, 3):
                x_copy(rel, y, 1).start()

    def first_mix(pair):
        for half, cos, sin in first(16 + pair):
            for side in range(2):
                at = ((half * 2 + side) * 8 + pair) * MIX_PITCH
                sign = 1.0 if side == 1 else -1.0
                value = cos[:, :128] + sign * sin[:, 128:]
                for i in range(10):
                    rows = slice(rows_at(side, i), rows_at(side, i) + 16)
                    xsm[pl.ds(pl.multiple_of(at + 16 * i, 8), 16), :] = value[rows]
        for rel in (2, 1, 3):
            xm_copy(rel, pair, 0).start()

    tables[0].wait()
    for load in loads(0):
        load.wait()
    for table in tables[1:4]:
        table.wait()
    for table in tables[4:6]:
        table.start()
    for load in loads(1):
        load.start()
    for table in tables[6:]:
        table.start()

    def produce(step, carry):
        @pl.when(step == 8)
        def _():
            for load in loads(1):
                load.wait()

        @pl.when(step < 16)
        def _():
            depth_main(step)

        @pl.when(step != 1)
        def _():
            first_main(jnp.maximum(step - 1, 0))

        @pl.when(step == 0)
        def _():
            for table in tables[4:6]:
                table.wait()

        @pl.when(step < 16)
        def _():
            depth_tail(step)

        return carry

    lax.fori_loop(0, 17, produce, 0)

    def produce_mix(pair, carry):
        first_mix(pair)
        return carry

    lax.fori_loop(0, 8, produce_mix, 0)

    def send_x(phase):
        group, octet, until, with_mix = PHASES[phase]

        def go(y, carry):
            for rel in (2, 1, 3):
                x_copy(rel, y, phase).start()
            return carry

        if until > octet:
            lax.fori_loop(EARLY if phase == 1 else 8 * octet, 8 * until, go, 0)

        def go_mix(pair, carry):
            for rel in (2, 1, 3):
                xm_copy(rel, pair, phase).start()
            return carry

        if with_mix:
            lax.fori_loop(0, 8, go_mix, 0)

    def d_span(phase):
        group, octet, until, with_mix = PHASES[phase]
        first_row, last_row = 32 * octet, 80 if with_mix else 32 * until
        return pl.ds(STARTS[group], GROUPS[group]), first_row, last_row - first_row

    def d_copy(phase, device, other):
        span, row, count = d_span(phase)
        src = dall.at[other, span, pl.ds(row, count)]
        place = pl.ds(pl.multiple_of(plane * 80 + row, 8), count)
        if PHASES[phase][0] == LAST:
            dst = ylast.at[:, place, :]
        else:
            dst = yall.at[span, place, :]
        if device is None:
            return pltpu.make_async_copy(src, dst, dl_sem.at[phase])
        return pltpu.make_async_remote_copy(
            src_ref=src,
            dst_ref=dst,
            send_sem=ds_sem.at[phase],
            recv_sem=dr_sem.at[phase],
            device_id=device,
            device_id_type=MESH,
        )

    def d_wait(phase, sem):
        span, row, count = d_span(phase)
        whole = dall.at[pl.ds(0, 15), span, pl.ds(row, count)]
        pltpu.make_async_copy(whole, whole, sem.at[phase]).wait()

    def turn(phase):
        group, first_octet, until, with_mix = PHASES[phase]
        i0, count = STARTS[group], GROUPS[group]

        def go(r, carry):
            i, place = i0 + r // 16, r % 16
            other = lo * place + (1 - lo) * (15 - place)

            def put(octet, offset, near_value, far_value):
                pitch, base = (16, 16, 8)[octet], 32 * octet + offset
                dall[other, i, pl.ds(pl.multiple_of(lo * pitch + base, 8), 8), :] = near_value
                dall[other, i, pl.ds(pl.multiple_of((1 - lo) * pitch + base, 8), 8), :] = far_value

            for octet in range(first_octet, until):
                for part in range(2):
                    base = octet * 8 * PITCH + 32 * i0 + part * 16 * count + r

                    def take(ref, item):
                        return ref[pl.ds(item * 16 * PITCH + base, 8, stride=PITCH), :]

                    put(octet, part * 8, take(xs, own) + take(xr, 1), take(xr, 0) + take(xr, 2))

            def take_mix(ref, item):
                return ref[pl.ds(item * 8 * MIX_PITCH + 16 * i0 + r, 8, stride=MIX_PITCH), :]

            if with_mix:
                put(2, 0, take_mix(xsm, own) + take_mix(xrm, 1), take_mix(xrm, 0) + take_mix(xrm, 2))
            return carry

        lax.fori_loop(0, 16 * count, go, 0)

    def x_wait(phase, sem):
        group, octet, until, with_mix = PHASES[phase]
        main = xr.at[pl.ds(0, 256 * (until - octet) * GROUPS[group]), :]
        mix = xrm.at[pl.ds(0, 128 * GROUPS[group]), :]
        for rel in range(3):
            if until > octet:
                pltpu.make_async_copy(main, main, sem.at[0, rel, phase]).wait()
            if with_mix:
                pltpu.make_async_copy(mix, mix, sem.at[1, rel, phase]).wait()

    lines = fields.reshape(24576, 128)

    def y_load(i):
        return pltpu.make_async_copy(
            yall.at[i], lines.at[pl.ds(pl.multiple_of(i * 1280, 1280), 1280), :], y_sem.at[i]
        )

    def part_copy(i):
        return pltpu.make_async_copy(rows.at[i % 2], parts.at[i], p_sem.at[i])

    def second(group):
        for phase in range(len(PHASES)):
            if PHASES[phase][0] == group:
                d_wait(phase, dr_sem)
                d_copy(phase, None, plane).wait()
        first_i, last_i = STARTS[group], STARTS[group] + GROUPS[group]
        if group < LAST:
            for i in range(first_i, last_i):
                y_load(i).start()

        def go(i, carry):
            if group < LAST:
                y_load(i).wait()

            @pl.when(i >= 2)
            def _():
                part_copy(i - 2).wait()

            def lift(offsets):
                return jnp.concatenate(
                    [
                        lines[pl.ds(pl.multiple_of(i * 1280 + 80 * j + offset, 8), 8), :]
                        if group < LAST
                        else ylast[0, 80 * j + offset : 80 * j + offset + 8, :]
                        for j in range(16)
                        for offset in offsets
                    ],
                    axis=0,
                )

            second_rows(lift, fth, ftl, rows.at[i % 2], slab * 10 + i)
            part_copy(i).start()
            return carry

        lax.fori_loop(first_i, last_i, go, 0)

    for phase in range(len(PHASES)):
        if phase + 1 < len(PHASES):
            send_x(phase + 1)
        x_wait(phase, xr_sem)
        turn(phase)
        for step in STEPS:
            other, device = peer_plane(step)
            d_copy(phase, device, other).start()
        d_copy(phase, None, plane).start()
        if phase == 0:
            for table in tables[6:]:
                table.wait()
        elif phase < len(GROUPS):
            second(phase - 1)

    def z_left(chunk, carry):
        z_copy(chunk).wait_send()
        return carry

    lax.fori_loop(12, 16, z_left, 0)
    lax.fori_loop(22, 24, z_left, 0)
    for phase in range(len(PHASES)):
        x_wait(phase, xs_sem)
    second(len(GROUPS) - 1)
    for phase in range(len(PHASES)):
        d_wait(phase, ds_sem)
    part_copy(8).wait()
    part_copy(9).wait()


def exchange(u, v, t):
    zh, zl = depth_tables()
    xh, xl = first_tables()
    fh, fl = second_tables()
    phases = len(PHASES)
    any_space = pl.BlockSpec(memory_space=pl.ANY)
    return pl.pallas_call(
        exchange_kernel,
        out_shape=(
            jax.ShapeDtypeStruct((9, 1280, 128), F32),
            jax.ShapeDtypeStruct((10, 3, 320, 128), F32),
        ),
        in_specs=[any_space] * 9,
        out_specs=(any_space, any_space),
        scratch_shapes=[
            pltpu.VMEM((3, 4, 2, 128, 8, 128), F32),
            pltpu.VMEM((3, 512, 256), BF16),
            pltpu.VMEM((3, 512, 256), BF16),
            pltpu.VMEM((352, 256), BF16),
            pltpu.VMEM((352, 256), BF16),
            pltpu.VMEM((2, 2, 320, 256), BF16),
            pltpu.VMEM((2, 2, 320, 256), BF16),
            pltpu.VMEM((1024, 512), BF16),
            pltpu.VMEM((512, 256), F32),
            pltpu.VMEM((24, 2, 256, 256), F32),
            pltpu.VMEM((6, 2, 128, 256), F32),
            pltpu.VMEM((4 * 16 * PITCH, 128), F32),
            pltpu.VMEM((3 * 16 * PITCH, 128), F32),
            pltpu.VMEM((4 * 8 * MIX_PITCH, 128), F32),
            pltpu.VMEM((3 * 8 * MIX_PITCH, 128), F32),
            pltpu.VMEM((16, 10, 80, 128), F32),
            pltpu.VMEM((1, 1280, 128), F32),
            pltpu.VMEM((2, 3, 320, 128), F32),
            pltpu.SemaphoreType.DMA((2, 3, 4)),
            pltpu.SemaphoreType.DMA((8,)),
            pltpu.SemaphoreType.DMA((24,)),
            pltpu.SemaphoreType.DMA((24,)),
            pltpu.SemaphoreType.DMA((2, 3, phases)),
            pltpu.SemaphoreType.DMA((2, 3, phases)),
            pltpu.SemaphoreType.DMA((phases,)),
            pltpu.SemaphoreType.DMA((phases,)),
            pltpu.SemaphoreType.DMA((phases,)),
            pltpu.SemaphoreType.DMA((10,)),
            pltpu.SemaphoreType.DMA((10,)),
        ],
        compiler_params=pltpu.CompilerParams(
            collective_id=0, has_side_effects=True, vmem_limit_bytes=67043328
        ),
        name="exchange",
    )(u, v, t, zh, zl, xh, xl, fh, fl)


def lay_out_kernel(parts, out):
    for i in range(5):
        out[0, i, :, :128] = parts[i, 0]
        out[0, i, :, 128:256] = parts[i, 1]
        out[0, i, :, 256:] = parts[i, 2, :, :64]


def lay_out(parts):
    return pl.pallas_call(
        lay_out_kernel,
        grid=(2,),
        out_shape=jax.ShapeDtypeStruct((1, 10, 320, 320), F32),
        in_specs=[pl.BlockSpec((5, 3, 320, 128), lambda i: (i, 0, 0, 0))],
        out_specs=pl.BlockSpec((1, 5, 320, 320), lambda i: (0, i, 0, 0)),
        compiler_params=pltpu.CompilerParams(dimension_semantics=("arbitrary",)),
        name="lay_out",
    )(parts)


def shards(velocity_u, velocity_v, scalar_theta):
    return lay_out(exchange(velocity_u, velocity_v, scalar_theta)[1])


def solution(mesh):
    spec = P("field", "slab", None)
    return jax.shard_map(
        shards,
        mesh=mesh,
        in_specs=(spec, spec, spec),
        out_specs=P("field", "slab", None, None),
        check_vma=False,
    )
```

```python
import functools

import jax
import jax.numpy as jnp
import numpy as np
from jax import lax
from jax.experimental import pallas as pl
from jax.experimental.pallas import tpu as pltpu
from jax.sharding import PartitionSpec as P

N = 512
KEEP = 160
MESH = pl.DeviceIdType.MESH
F32 = jnp.float32
BF16 = jnp.bfloat16
GROUPS = (3, 2, 2, 1, 1, 1)
STARTS = (0, 3, 5, 7, 8, 9)
LAST = 5
PHASES = (
    ((0, 0, 2, True), (1, 0, 2, True), (2, 0, 2, True), (3, 0, 2, True), (4, 0, 2, True))
    + ((5, 0, 1, False), (5, 1, 2, False), (5, 2, 2, True))
)
STEPS = (
    ((0, 1), (1, 0), (0, 3), (3, 0), (1, 1), (3, 3), (1, 3), (3, 1))
    + ((2, 1), (2, 3), (0, 2), (2, 0), (2, 2))
    + ((1, 2), (3, 2))
)
EARLY = 8
PITCH = 328
MIX_PITCH = 168
FACTORS = ((0, 0), (1, 1), (0, 1), (0, 2))


def split_table(table):
    high = table.astype(BF16)
    low = (table - high.astype(np.float64)).astype(BF16)
    return high, low


def waves(k, x):
    angle = (np.outer(k, x) % N) * (2.0 * np.pi / N)
    return np.cos(angle) / np.sqrt(N), np.sin(angle) / np.sqrt(N)


def depth_tables():
    cos, sin = waves(np.arange(KEEP), np.arange(N))
    real, imag = cos.T, -sin.T
    tables = np.zeros((3, N, 256))
    tables[0, :, :128] = real[:, :128]
    tables[0, :, 128:] = imag[:, :128]
    for parity in range(2):
        at = 64 * parity
        tables[1 + parity, :, at : at + 32] = real[:, 128:]
        tables[1 + parity, :, at + 32 : at + 64] = imag[:, 128:]
        tables[1 + parity, :, at + 128 : at + 160] = imag[:, 128:]
        tables[1 + parity, :, at + 160 : at + 192] = -real[:, 128:]
    return split_table(tables)


def first_tables():
    order = (10 * np.arange(16)[None, :] + np.arange(11)[:, None]).reshape(-1)
    tables = np.zeros((2, 352, 256))
    for half in range(2):
        tables[half] = np.concatenate(waves(order, np.arange(256) + 256 * half), axis=0)
    return split_table(tables)


def second_tables():
    tables = np.zeros((2, 2, 320, 256))
    y = np.arange(256)
    mixed = np.concatenate([2 * np.arange(128), 2 * np.arange(128) + 1])
    for parity in range(2):
        k = 2 * np.arange(KEEP) + parity - KEEP
        for order, places in enumerate((y, mixed)):
            cos, sin = waves(k, places)
            tables[parity, order] = np.concatenate([cos, sin], axis=0)
    return split_table(tables)


def halves(value):
    high = value.astype(BF16)
    return high, (value - high.astype(F32)).astype(BF16)


def dot(a, b):
    return jnp.dot(a, b, preferred_element_type=F32)


def second_rows(lift, fh, fl, rows, row):
    real_of = [lift((16 * a, 32 + 16 * a)) for a in range(2)]
    imag_of = [lift((16 * a + 8, 40 + 16 * a)) for a in range(2)]
    tail_of = [lift((64 + 8 * a,)) for a in range(2)]
    for parity in range(2):

        def fold(pair):
            return pair[0] + pair[1] if parity == 0 else pair[0] - pair[1]

        part = jnp.concatenate([fold(real_of), fold(imag_of)], axis=1)
        tail = fold(tail_of)
        tail = jnp.concatenate([tail, pltpu.roll(tail, 64, 1)], axis=0)
        outs = []
        for order, value in ((0, part), (1, tail)):
            high, low = halves(value)
            a, b = fh[parity, order], fl[parity, order]
            outs.append(dot(a, high) + dot(a, low) + dot(b, high))
        wide, slim = outs
        cos, sin = wide[:160], wide[160:]
        real = cos[:, :128] + sin[:, 128:]
        imag = cos[:, 128:] - sin[:, :128]
        cos, sin = slim[:160], slim[160:]
        tail_real = cos + pltpu.roll(sin, 96, 1)
        tail_imag = cos - pltpu.roll(sin, 32, 1)
        result = jnp.concatenate(
            [real, tail_real[:, :32], imag, tail_imag[:, 32:64], jnp.zeros((160, 64), F32)], axis=1
        )
        if parity == 0:
            at_row = lax.broadcasted_iota(jnp.int32, (160, 384), 0)
            at_col = lax.broadcasted_iota(jnp.int32, (160, 384), 1)
            zero = (at_row == 80) & (at_col == 0) & (row == KEEP)
            result = jnp.where(zero, 0.0, result)
        for place in range(3):
            rows[place, pl.ds(parity, 160, stride=2), :] = result[:, place * 128 : place * 128 + 128]


def exchange_kernel(
    u, v, t, zh, zl, xh, xl, fh, fl, yall, parts,
    fields, zth, ztl, xth, xtl, fth, ftl, stack, held, zbuf, zout, xs, xr, xsm, xrm, dall, ylast, rows,
    in_sem, tab_sem, zs_sem, zr_sem, xs_sem, xr_sem, ds_sem, dr_sem, dl_sem, y_sem, p_sem,
):
    field, slab = lax.axis_index("field"), lax.axis_index("slab")
    hi, core = field // 2, field % 2
    lo, plane = slab // 16, slab % 16
    own = hi * 2 + lo

    def peer_x(rel):
        half, side = (hi + rel // 2) % 2, (lo + rel % 2) % 2
        return half, side, {"field": half * 2 + core, "slab": side * 16 + plane}

    def peer_plane(step):
        other = (plane // 4 + step[0]) % 4 * 4 + (plane + step[1]) % 4
        return other, {"field": field, "slab": lo * 16 + other}

    partner = {"field": hi * 2 + (1 - core), "slab": slab}

    def loads(octet):
        return [
            pltpu.make_async_copy(
                ref.at[:, pl.ds(8 * octet, 8), pl.ds(128 * part, 128)],
                fields.at[i, part, octet],
                in_sem.at[octet, i, part],
            )
            for part in range(4)
            for i, ref in enumerate((u, v, t))
        ]

    tables = [
        pltpu.make_async_copy(src, dst, tab_sem.at[i])
        for i, (src, dst) in enumerate(
            (
                (zh.at[0], zth.at[0]), (zl.at[0], ztl.at[0]), (xh.at[hi], xth), (xl.at[hi], xtl),
                (zh.at[pl.ds(1, 2)], zth.at[pl.ds(1, 2)]), (zl.at[pl.ds(1, 2)], ztl.at[pl.ds(1, 2)]),
                (fh, fth), (fl, ftl),
            )
        )
    ]
    tables[0].start()
    tables[1].start()
    for load in loads(0):
        load.start()
    for table in tables[2:4]:
        table.start()

    barrier = pltpu.get_barrier_semaphore()
    pl.semaphore_signal(barrier, 1, device_id=partner, device_id_type=MESH)
    for rel in range(1, 4):
        pl.semaphore_signal(barrier, 1, device_id=peer_x(rel)[2], device_id_type=MESH)

    for step in STEPS:
        pl.semaphore_signal(barrier, 1, device_id=peer_plane(step)[1], device_id_type=MESH)
    pl.semaphore_wait(barrier, 19)

    def z_slot(chunk):
        return jnp.where(chunk < 16, chunk % 4, 4 + chunk % 2)

    def z_copy(chunk):
        return pltpu.make_async_remote_copy(
            src_ref=zout.at[z_slot(chunk)],
            dst_ref=zbuf.at[chunk, :, pl.ds(pl.multiple_of(core * 128, 128), 128), :],
            send_sem=zs_sem.at[chunk],
            recv_sem=zr_sem.at[chunk],
            device_id=partner,
            device_id_type=MESH,
        )

    def put_z(chunk, value):
        rows = pl.ds(pl.multiple_of(core * 128, 128), 128)
        for half in range(2):
            zbuf[chunk, half, rows, :] = value[half * 128 : half * 128 + 128]
            zout[z_slot(chunk), half] = value[256 + half * 128 : 384 + half * 128]
        z_copy(chunk).start()

    flat = fields.reshape(3, 4, 2048, 128)

    def depth_by(table):
        both = dot(stack[...], zth[table])
        return both[:512] + both[512:] + dot(stack[:512], ztl[table])

    def depth_main(y):
        for part in range(4):
            rows = pl.ds((y // 8) * 1024 + y % 8, 128, stride=8)
            values = [flat[i, part, rows, :] for i in range(3)]
            columns = slice(part * 128, part * 128 + 128)
            for product, (a, b) in enumerate(FACTORS):
                high, low = halves(values[a] * values[b])
                row = (product + core) % 2 * 256 + product // 2 * 128
                stack[pl.ds(pl.multiple_of(row, 128), 128), columns] = high
                stack[pl.ds(pl.multiple_of(row + 512, 128), 128), columns] = low

        @pl.when(y >= 4)
        def _():
            z_copy(y - 4).wait_send()

        put_z(y, depth_by(0))

    def depth_tail(y):
        tail = depth_by(1 + y % 2)

        @pl.when(y % 2 == 0)
        def _():
            held[...] = tail

        @pl.when(y % 2 == 1)
        def _():
            @pl.when(y >= 4)
            def _():
                z_copy(16 + y // 2 - 2).wait_send()

            put_z(16 + y // 2, held[...] + tail)

    def first(chunk):
        z_copy(chunk).wait_recv()
        pairs = []
        for half in range(2):
            high, low = halves(zbuf[chunk, half])
            mixed = dot(xth[...], high) + dot(xth[...], low) + dot(xtl[...], high)
            pairs.append((half, mixed[:176], mixed[176:]))
        return pairs

    def rows_at(side, i):
        return 16 * i if side == 1 else 16 * (10 - i)

    def x_copy(rel, y, phase):
        half, side, device = peer_x(rel)
        group = PHASES[phase][0]
        at, count = 32 * STARTS[group], 32 * GROUPS[group]

        def rows(item):
            return pl.ds(pl.multiple_of(item * PITCH + at, 8), count)

        return pltpu.make_async_remote_copy(
            src_ref=xs.at[rows((half * 2 + side) * 16 + y), :],
            dst_ref=xr.at[rows((rel - 1) * 16 + y), :],
            send_sem=xs_sem.at[0, rel - 1, phase],
            recv_sem=xr_sem.at[0, rel - 1, phase],
            device_id=device,
            device_id_type=MESH,
        )

    def xm_copy(rel, pair, phase):
        half, side, device = peer_x(rel)
        group = PHASES[phase][0]
        at, count = 16 * STARTS[group], 16 * GROUPS[group]

        def rows(item):
            return pl.ds(pl.multiple_of(item * MIX_PITCH + at, 8), count)

        return pltpu.make_async_remote_copy(
            src_ref=xsm.at[rows((half * 2 + side) * 8 + pair), :],
            dst_ref=xrm.at[rows((rel - 1) * 8 + pair), :],
            send_sem=xs_sem.at[1, rel - 1, phase],
            recv_sem=xr_sem.at[1, rel - 1, phase],
            device_id=device,
            device_id_type=MESH,
        )

    def first_main(y):
        for half, cos, sin in first(y):
            for side in range(2):
                base = ((half * 2 + side) * 16 + y) * PITCH
                sign = 1.0 if side == 1 else -1.0
                real = cos[:, :128] + sign * sin[:, 128:]
                imag = cos[:, 128:] - sign * sin[:, :128]
                for i0, count in zip(STARTS, GROUPS):
                    at = base + 32 * i0
                    for i in range(count):
                        rows = slice(rows_at(side, i0 + i), rows_at(side, i0 + i) + 16)
                        xs[pl.ds(pl.multiple_of(at + 16 * i, 8), 16), :] = real[rows]
                        xs[pl.ds(pl.multiple_of(at + 16 * (count + i), 8), 16), :] = imag[rows]
        for rel in (1, 3, 2):
            x_copy(rel, y, 0).start()

        @pl.when(y < EARLY)
        def _():
            for rel in (1, 3, 2):
                x_copy(rel, y, 1).start()

    def first_mix(pair):
        for half, cos, sin in first(16 + pair):
            for side in range(2):
                at = ((half * 2 + side) * 8 + pair) * MIX_PITCH
                sign = 1.0 if side == 1 else -1.0
                value = cos[:, :128] + sign * sin[:, 128:]
                for i in range(10):
                    rows = slice(rows_at(side, i), rows_at(side, i) + 16)
                    xsm[pl.ds(pl.multiple_of(at + 16 * i, 8), 16), :] = value[rows]
        for rel in (1, 3, 2):
            xm_copy(rel, pair, 0).start()

    tables[0].wait()
    for load in loads(0):
        load.wait()
    for table in tables[1:4]:
        table.wait()
    for table in tables[4:6]:
        table.start()
    for load in loads(1):
        load.start()
    for table in tables[6:]:
        table.start()

    def produce(step, carry):
        @pl.when(step == 8)
        def _():
            for load in loads(1):
                load.wait()

        @pl.when(step < 16)
        def _():
            depth_main(step)

        @pl.when(step != 1)
        def _():
            first_main(jnp.maximum(step - 1, 0))

        @pl.when(step == 0)
        def _():
            for table in tables[4:6]:
                table.wait()

        @pl.when(step < 16)
        def _():
            depth_tail(step)

        return carry

    lax.fori_loop(0, 17, produce, 0)

    def produce_mix(pair, carry):
        first_mix(pair)
        return carry

    lax.fori_loop(0, 8, produce_mix, 0)

    def send_x(phase):
        group, octet, until, with_mix = PHASES[phase]

        def go(y, carry):
            for rel in (1, 3, 2):
                x_copy(rel, y, phase).start()
            return carry

        if until > octet:
            lax.fori_loop(EARLY if phase == 1 else 8 * octet, 8 * until, go, 0)

        def go_mix(pair, carry):
            for rel in (1, 3, 2):
                xm_copy(rel, pair, phase).start()
            return carry

        if with_mix:
            lax.fori_loop(0, 8, go_mix, 0)

    def d_span(phase):
        group, octet, until, with_mix = PHASES[phase]
        first_row, last_row = 32 * octet, 80 if with_mix else 32 * until
        return pl.ds(STARTS[group], GROUPS[group]), first_row, last_row - first_row

    def d_copy(phase, device, other):
        span, row, count = d_span(phase)
        src = dall.at[other, span, pl.ds(row, count)]
        place = pl.ds(pl.multiple_of(plane * 80 + row, 8), count)
        if PHASES[phase][0] == LAST:
            dst = ylast.at[:, place, :]
        else:
            dst = yall.at[span, place, :]
        if device is None:
            return pltpu.make_async_copy(src, dst, dl_sem.at[phase])
        return pltpu.make_async_remote_copy(
            src_ref=src,
            dst_ref=dst,
            send_sem=ds_sem.at[phase],
            recv_sem=dr_sem.at[phase],
            device_id=device,
            device_id_type=MESH,
        )

    def d_wait(phase, sem):
        span, row, count = d_span(phase)
        whole = dall.at[pl.ds(0, 15), span, pl.ds(row, count)]
        pltpu.make_async_copy(whole, whole, sem.at[phase]).wait()

    def turn(phase):
        group, first_octet, until, with_mix = PHASES[phase]
        i0, count = STARTS[group], GROUPS[group]

        def go(r, carry):
            i, place = i0 + r // 16, r % 16
            other = lo * place + (1 - lo) * (15 - place)

            def put(octet, offset, near_value, far_value):
                pitch, base = (16, 16, 8)[octet], 32 * octet + offset
                dall[other, i, pl.ds(pl.multiple_of(lo * pitch + base, 8), 8), :] = near_value
                dall[other, i, pl.ds(pl.multiple_of((1 - lo) * pitch + base, 8), 8), :] = far_value

            for octet in range(first_octet, until):
                for part in range(2):
                    base = octet * 8 * PITCH + 32 * i0 + part * 16 * count + r

                    def take(ref, item):
                        return ref[pl.ds(item * 16 * PITCH + base, 8, stride=PITCH), :]

                    put(octet, part * 8, take(xs, own) + take(xr, 1), take(xr, 0) + take(xr, 2))

            def take_mix(ref, item):
                return ref[pl.ds(item * 8 * MIX_PITCH + 16 * i0 + r, 8, stride=MIX_PITCH), :]

            if with_mix:
                put(2, 0, take_mix(xsm, own) + take_mix(xrm, 1), take_mix(xrm, 0) + take_mix(xrm, 2))
            return carry

        lax.fori_loop(0, 16 * count, go, 0)

    def x_wait(phase, sem):
        group, octet, until, with_mix = PHASES[phase]
        main = xr.at[pl.ds(0, 256 * (until - octet) * GROUPS[group]), :]
        mix = xrm.at[pl.ds(0, 128 * GROUPS[group]), :]
        for rel in range(3):
            if until > octet:
                pltpu.make_async_copy(main, main, sem.at[0, rel, phase]).wait()
            if with_mix:
                pltpu.make_async_copy(mix, mix, sem.at[1, rel, phase]).wait()

    lines = fields.reshape(24576, 128)

    def y_load(i):
        return pltpu.make_async_copy(
            yall.at[i], lines.at[pl.ds(pl.multiple_of(i * 1280, 1280), 1280), :], y_sem.at[i]
        )

    def part_copy(i):
        return pltpu.make_async_copy(rows.at[i % 2], parts.at[i], p_sem.at[i])

    def second(group):
        for phase in range(len(PHASES)):
            if PHASES[phase][0] == group:
                d_wait(phase, dr_sem)
                d_copy(phase, None, plane).wait()
        first_i, last_i = STARTS[group], STARTS[group] + GROUPS[group]
        if group < LAST:
            for i in range(first_i, last_i):
                y_load(i).start()

        def go(i, carry):
            if group < LAST:
                y_load(i).wait()

            @pl.when(i >= 2)
            def _():
                part_copy(i - 2).wait()

            def lift(offsets):
                return jnp.concatenate(
                    [
                        lines[pl.ds(pl.multiple_of(i * 1280 + 80 * j + offset, 8), 8), :]
                        if group < LAST
                        else ylast[0, 80 * j + offset : 80 * j + offset + 8, :]
                        for j in range(16)
                        for offset in offsets
                    ],
                    axis=0,
                )

            second_rows(lift, fth, ftl, rows.at[i % 2], slab * 10 + i)
            part_copy(i).start()
            return carry

        lax.fori_loop(first_i, last_i, go, 0)

    for phase in range(len(PHASES)):
        if phase + 1 < len(PHASES):
            send_x(phase + 1)
        x_wait(phase, xr_sem)
        turn(phase)
        for step in STEPS:
            other, device = peer_plane(step)
            d_copy(phase, device, other).start()
        d_copy(phase, None, plane).start()
        if phase == 0:
            for table in tables[6:]:
                table.wait()
        elif 2 <= phase <= LAST + 1:
            second(phase - 2)

    def z_left(chunk, carry):
        z_copy(chunk).wait_send()
        return carry

    lax.fori_loop(12, 16, z_left, 0)
    lax.fori_loop(22, 24, z_left, 0)
    for phase in range(len(PHASES)):
        x_wait(phase, xs_sem)
    second(len(GROUPS) - 1)
    for phase in range(len(PHASES)):
        d_wait(phase, ds_sem)
    part_copy(8).wait()
    part_copy(9).wait()


def exchange(u, v, t):
    zh, zl = depth_tables()
    xh, xl = first_tables()
    fh, fl = second_tables()
    phases = len(PHASES)
    any_space = pl.BlockSpec(memory_space=pl.ANY)
    return pl.pallas_call(
        exchange_kernel,
        out_shape=(
            jax.ShapeDtypeStruct((9, 1280, 128), F32),
            jax.ShapeDtypeStruct((10, 3, 320, 128), F32),
        ),
        in_specs=[any_space] * 9,
        out_specs=(any_space, any_space),
        scratch_shapes=[
            pltpu.VMEM((3, 4, 2, 128, 8, 128), F32),
            pltpu.VMEM((3, 512, 256), BF16),
            pltpu.VMEM((3, 512, 256), BF16),
            pltpu.VMEM((352, 256), BF16),
            pltpu.VMEM((352, 256), BF16),
            pltpu.VMEM((2, 2, 320, 256), BF16),
            pltpu.VMEM((2, 2, 320, 256), BF16),
            pltpu.VMEM((1024, 512), BF16),
            pltpu.VMEM((512, 256), F32),
            pltpu.VMEM((24, 2, 256, 256), F32),
            pltpu.VMEM((6, 2, 128, 256), F32),
            pltpu.VMEM((4 * 16 * PITCH, 128), F32),
            pltpu.VMEM((3 * 16 * PITCH, 128), F32),
            pltpu.VMEM((4 * 8 * MIX_PITCH, 128), F32),
            pltpu.VMEM((3 * 8 * MIX_PITCH, 128), F32),
            pltpu.VMEM((16, 10, 80, 128), F32),
            pltpu.VMEM((1, 1280, 128), F32),
            pltpu.VMEM((2, 3, 320, 128), F32),
            pltpu.SemaphoreType.DMA((2, 3, 4)),
            pltpu.SemaphoreType.DMA((8,)),
            pltpu.SemaphoreType.DMA((24,)),
            pltpu.SemaphoreType.DMA((24,)),
            pltpu.SemaphoreType.DMA((2, 3, phases)),
            pltpu.SemaphoreType.DMA((2, 3, phases)),
            pltpu.SemaphoreType.DMA((phases,)),
            pltpu.SemaphoreType.DMA((phases,)),
            pltpu.SemaphoreType.DMA((phases,)),
            pltpu.SemaphoreType.DMA((10,)),
            pltpu.SemaphoreType.DMA((10,)),
        ],
        compiler_params=pltpu.CompilerParams(
            collective_id=0, has_side_effects=True, vmem_limit_bytes=67043328
        ),
        name="exchange",
    )(u, v, t, zh, zl, xh, xl, fh, fl)


def lay_out_kernel(parts, out):
    for i in range(5):
        out[0, i, :, :128] = parts[i, 0]
        out[0, i, :, 128:256] = parts[i, 1]
        out[0, i, :, 256:] = parts[i, 2, :, :64]


def lay_out(parts):
    return pl.pallas_call(
        lay_out_kernel,
        grid=(2,),
        out_shape=jax.ShapeDtypeStruct((1, 10, 320, 320), F32),
        in_specs=[pl.BlockSpec((5, 3, 320, 128), lambda i: (i, 0, 0, 0))],
        out_specs=pl.BlockSpec((1, 5, 320, 320), lambda i: (0, i, 0, 0)),
        compiler_params=pltpu.CompilerParams(dimension_semantics=("arbitrary",)),
        name="lay_out",
    )(parts)


def shards(velocity_u, velocity_v, scalar_theta):
    return lay_out(exchange(velocity_u, velocity_v, scalar_theta)[1])


def solution(mesh):
    spec = P("field", "slab", None)
    return jax.shard_map(
        shards,
        mesh=mesh,
        in_specs=(spec, spec, spec),
        out_specs=P("field", "slab", None, None),
        check_vma=False,
    )
```

```python
import functools

import jax
import jax.numpy as jnp
import numpy as np
from jax import lax
from jax.experimental import pallas as pl
from jax.experimental.pallas import tpu as pltpu
from jax.sharding import PartitionSpec as P

N = 512
KEEP = 160
MESH = pl.DeviceIdType.MESH
F32 = jnp.float32
BF16 = jnp.bfloat16
GROUPS = (3, 2, 2, 1, 1, 1)
STARTS = (0, 3, 5, 7, 8, 9)
LAST = 5
PHASES = (
    ((0, 0, 2, True), (1, 0, 2, True), (2, 0, 2, True), (3, 0, 2, True), (4, 0, 2, True))
    + ((5, 0, 1, False), (5, 1, 2, False), (5, 2, 2, True))
)
STEPS = (
    ((0, 1), (1, 0), (0, 3), (3, 0), (1, 1), (3, 3), (1, 3), (3, 1))
    + ((2, 1), (2, 3), (0, 2), (2, 0), (2, 2))
    + ((1, 2), (3, 2))
)
EARLY = 4
PITCH = 328
MIX_PITCH = 168
FACTORS = ((0, 0), (1, 1), (0, 1), (0, 2))


def split_table(table):
    high = table.astype(BF16)
    low = (table - high.astype(np.float64)).astype(BF16)
    return high, low


def waves(k, x):
    angle = (np.outer(k, x) % N) * (2.0 * np.pi / N)
    return np.cos(angle) / np.sqrt(N), np.sin(angle) / np.sqrt(N)


def depth_tables():
    cos, sin = waves(np.arange(KEEP), np.arange(N))
    real, imag = cos.T, -sin.T
    tables = np.zeros((3, N, 256))
    tables[0, :, :128] = real[:, :128]
    tables[0, :, 128:] = imag[:, :128]
    for parity in range(2):
        at = 64 * parity
        tables[1 + parity, :, at : at + 32] = real[:, 128:]
        tables[1 + parity, :, at + 32 : at + 64] = imag[:, 128:]
        tables[1 + parity, :, at + 128 : at + 160] = imag[:, 128:]
        tables[1 + parity, :, at + 160 : at + 192] = -real[:, 128:]
    return split_table(tables)


def first_tables():
    order = (10 * np.arange(16)[None, :] + np.arange(11)[:, None]).reshape(-1)
    tables = np.zeros((2, 352, 256))
    for half in range(2):
        tables[half] = np.concatenate(waves(order, np.arange(256) + 256 * half), axis=0)
    return split_table(tables)


def second_tables():
    tables = np.zeros((2, 2, 320, 256))
    y = np.arange(256)
    mixed = np.concatenate([2 * np.arange(128), 2 * np.arange(128) + 1])
    for parity in range(2):
        k = 2 * np.arange(KEEP) + parity - KEEP
        for order, places in enumerate((y, mixed)):
            cos, sin = waves(k, places)
            tables[parity, order] = np.concatenate([cos, sin], axis=0)
    return split_table(tables)


def halves(value):
    high = value.astype(BF16)
    return high, (value - high.astype(F32)).astype(BF16)


def dot(a, b):
    return jnp.dot(a, b, preferred_element_type=F32)


def second_rows(lift, fh, fl, rows, row):
    real_of = [lift((16 * a, 32 + 16 * a)) for a in range(2)]
    imag_of = [lift((16 * a + 8, 40 + 16 * a)) for a in range(2)]
    tail_of = [lift((64 + 8 * a,)) for a in range(2)]
    for parity in range(2):

        def fold(pair):
            return pair[0] + pair[1] if parity == 0 else pair[0] - pair[1]

        part = jnp.concatenate([fold(real_of), fold(imag_of)], axis=1)
        tail = fold(tail_of)
        tail = jnp.concatenate([tail, pltpu.roll(tail, 64, 1)], axis=0)
        outs = []
        for order, value in ((0, part), (1, tail)):
            high, low = halves(value)
            a, b = fh[parity, order], fl[parity, order]
            outs.append(dot(a, high) + dot(a, low) + dot(b, high))
        wide, slim = outs
        cos, sin = wide[:160], wide[160:]
        real = cos[:, :128] + sin[:, 128:]
        imag = cos[:, 128:] - sin[:, :128]
        cos, sin = slim[:160], slim[160:]
        tail_real = cos + pltpu.roll(sin, 96, 1)
        tail_imag = cos - pltpu.roll(sin, 32, 1)
        result = jnp.concatenate(
            [real, tail_real[:, :32], imag, tail_imag[:, 32:64], jnp.zeros((160, 64), F32)], axis=1
        )
        if parity == 0:
            at_row = lax.broadcasted_iota(jnp.int32, (160, 384), 0)
            at_col = lax.broadcasted_iota(jnp.int32, (160, 384), 1)
            zero = (at_row == 80) & (at_col == 0) & (row == KEEP)
            result = jnp.where(zero, 0.0, result)
        for place in range(3):
            rows[place, pl.ds(parity, 160, stride=2), :] = result[:, place * 128 : place * 128 + 128]


def exchange_kernel(
    u, v, t, zh, zl, xh, xl, fh, fl, yall, parts,
    fields, zth, ztl, xth, xtl, fth, ftl, stack, held, zbuf, zout, xs, xr, xsm, xrm, dall, ylast, rows,
    in_sem, tab_sem, zs_sem, zr_sem, xs_sem, xr_sem, ds_sem, dr_sem, dl_sem, y_sem, p_sem,
):
    field, slab = lax.axis_index("field"), lax.axis_index("slab")
    hi, core = field // 2, field % 2
    lo, plane = slab // 16, slab % 16
    own = hi * 2 + lo

    def peer_x(rel):
        half, side = (hi + rel // 2) % 2, (lo + rel % 2) % 2
        return half, side, {"field": half * 2 + core, "slab": side * 16 + plane}

    def peer_plane(step):
        other = (plane // 4 + step[0]) % 4 * 4 + (plane + step[1]) % 4
        return other, {"field": field, "slab": lo * 16 + other}

    partner = {"field": hi * 2 + (1 - core), "slab": slab}

    def loads(octet):
        return [
            pltpu.make_async_copy(
                ref.at[:, pl.ds(8 * octet, 8), pl.ds(128 * part, 128)],
                fields.at[i, part, octet],
                in_sem.at[octet, i, part],
            )
            for part in range(4)
            for i, ref in enumerate((u, v, t))
        ]

    tables = [
        pltpu.make_async_copy(src, dst, tab_sem.at[i])
        for i, (src, dst) in enumerate(
            (
                (zh.at[0], zth.at[0]), (zl.at[0], ztl.at[0]), (xh.at[hi], xth), (xl.at[hi], xtl),
                (zh.at[pl.ds(1, 2)], zth.at[pl.ds(1, 2)]), (zl.at[pl.ds(1, 2)], ztl.at[pl.ds(1, 2)]),
                (fh, fth), (fl, ftl),
            )
        )
    ]
    tables[0].start()
    tables[1].start()
    for load in loads(0):
        load.start()
    for table in tables[2:4]:
        table.start()

    barrier = pltpu.get_barrier_semaphore()
    pl.semaphore_signal(barrier, 1, device_id=partner, device_id_type=MESH)
    for rel in range(1, 4):
        pl.semaphore_signal(barrier, 1, device_id=peer_x(rel)[2], device_id_type=MESH)

    for step in STEPS:
        pl.semaphore_signal(barrier, 1, device_id=peer_plane(step)[1], device_id_type=MESH)
    pl.semaphore_wait(barrier, 19)

    def z_slot(chunk):
        return jnp.where(chunk < 16, chunk % 4, 4 + chunk % 2)

    def z_copy(chunk):
        return pltpu.make_async_remote_copy(
            src_ref=zout.at[z_slot(chunk)],
            dst_ref=zbuf.at[chunk, :, pl.ds(pl.multiple_of(core * 128, 128), 128), :],
            send_sem=zs_sem.at[chunk],
            recv_sem=zr_sem.at[chunk],
            device_id=partner,
            device_id_type=MESH,
        )

    def put_z(chunk, value):
        rows = pl.ds(pl.multiple_of(core * 128, 128), 128)
        for half in range(2):
            zbuf[chunk, half, rows, :] = value[half * 128 : half * 128 + 128]
            zout[z_slot(chunk), half] = value[256 + half * 128 : 384 + half * 128]
        z_copy(chunk).start()

    flat = fields.reshape(3, 4, 2048, 128)

    def depth_by(table):
        both = dot(stack[...], zth[table])
        return both[:512] + both[512:] + dot(stack[:512], ztl[table])

    def depth_main(y):
        for part in range(4):
            rows = pl.ds((y // 8) * 1024 + y % 8, 128, stride=8)
            values = [flat[i, part, rows, :] for i in range(3)]
            columns = slice(part * 128, part * 128 + 128)
            for product, (a, b) in enumerate(FACTORS):
                high, low = halves(values[a] * values[b])
                row = (product + core) % 2 * 256 + product // 2 * 128
                stack[pl.ds(pl.multiple_of(row, 128), 128), columns] = high
                stack[pl.ds(pl.multiple_of(row + 512, 128), 128), columns] = low

        @pl.when(y >= 4)
        def _():
            z_copy(y - 4).wait_send()

        put_z(y, depth_by(0))

    def depth_tail(y):
        tail = depth_by(1 + y % 2)

        @pl.when(y % 2 == 0)
        def _():
            held[...] = tail

        @pl.when(y % 2 == 1)
        def _():
            @pl.when(y >= 4)
            def _():
                z_copy(16 + y // 2 - 2).wait_send()

            put_z(16 + y // 2, held[...] + tail)

    def first(chunk):
        z_copy(chunk).wait_recv()
        pairs = []
        for half in range(2):
            high, low = halves(zbuf[chunk, half])
            mixed = dot(xth[...], high) + dot(xth[...], low) + dot(xtl[...], high)
            pairs.append((half, mixed[:176], mixed[176:]))
        return pairs

    def rows_at(side, i):
        return 16 * i if side == 1 else 16 * (10 - i)

    def x_copy(rel, y, phase):
        half, side, device = peer_x(rel)
        group = PHASES[phase][0]
        at, count = 32 * STARTS[group], 32 * GROUPS[group]

        def rows(item):
            return pl.ds(pl.multiple_of(item * PITCH + at, 8), count)

        return pltpu.make_async_remote_copy(
            src_ref=xs.at[rows((half * 2 + side) * 16 + y), :],
            dst_ref=xr.at[rows((rel - 1) * 16 + y), :],
            send_sem=xs_sem.at[0, rel - 1, phase],
            recv_sem=xr_sem.at[0, rel - 1, phase],
            device_id=device,
            device_id_type=MESH,
        )

    def xm_copy(rel, pair, phase):
        half, side, device = peer_x(rel)
        group = PHASES[phase][0]
        at, count = 16 * STARTS[group], 16 * GROUPS[group]

        def rows(item):
            return pl.ds(pl.multiple_of(item * MIX_PITCH + at, 8), count)

        return pltpu.make_async_remote_copy(
            src_ref=xsm.at[rows((half * 2 + side) * 8 + pair), :],
            dst_ref=xrm.at[rows((rel - 1) * 8 + pair), :],
            send_sem=xs_sem.at[1, rel - 1, phase],
            recv_sem=xr_sem.at[1, rel - 1, phase],
            device_id=device,
            device_id_type=MESH,
        )

    def first_main(y):
        for half, cos, sin in first(y):
            for side in range(2):
                base = ((half * 2 + side) * 16 + y) * PITCH
                sign = 1.0 if side == 1 else -1.0
                real = cos[:, :128] + sign * sin[:, 128:]
                imag = cos[:, 128:] - sign * sin[:, :128]
                for i0, count in zip(STARTS, GROUPS):
                    at = base + 32 * i0
                    for i in range(count):
                        rows = slice(rows_at(side, i0 + i), rows_at(side, i0 + i) + 16)
                        xs[pl.ds(pl.multiple_of(at + 16 * i, 8), 16), :] = real[rows]
                        xs[pl.ds(pl.multiple_of(at + 16 * (count + i), 8), 16), :] = imag[rows]
        for rel in (1, 3, 2):
            x_copy(rel, y, 0).start()

        @pl.when(y < EARLY)
        def _():
            for rel in (1, 3, 2):
                x_copy(rel, y, 1).start()

    def first_mix(pair):
        for half, cos, sin in first(16 + pair):
            for side in range(2):
                at = ((half * 2 + side) * 8 + pair) * MIX_PITCH
                sign = 1.0 if side == 1 else -1.0
                value = cos[:, :128] + sign * sin[:, 128:]
                for i in range(10):
                    rows = slice(rows_at(side, i), rows_at(side, i) + 16)
                    xsm[pl.ds(pl.multiple_of(at + 16 * i, 8), 16), :] = value[rows]
        for rel in (1, 3, 2):
            xm_copy(rel, pair, 0).start()

    tables[0].wait()
    for load in loads(0):
        load.wait()
    for table in tables[1:4]:
        table.wait()
    for table in tables[4:6]:
        table.start()
    for load in loads(1):
        load.start()
    for table in tables[6:]:
        table.start()

    def produce(step, carry):
        @pl.when(step == 8)
        def _():
            for load in loads(1):
                load.wait()

        @pl.when(step < 16)
        def _():
            depth_main(step)

        @pl.when(step != 1)
        def _():
            first_main(jnp.maximum(step - 1, 0))

        @pl.when(step == 0)
        def _():
            for table in tables[4:6]:
                table.wait()

        @pl.when(step < 16)
        def _():
            depth_tail(step)

        return carry

    lax.fori_loop(0, 17, produce, 0)

    def produce_mix(pair, carry):
        first_mix(pair)
        return carry

    lax.fori_loop(0, 8, produce_mix, 0)

    def send_x(phase):
        group, octet, until, with_mix = PHASES[phase]

        def go(y, carry):
            for rel in (1, 3, 2):
                x_copy(rel, y, phase).start()
            return carry

        if until > octet:
            lax.fori_loop(EARLY if phase == 1 else 8 * octet, 8 * until, go, 0)

        def go_mix(pair, carry):
            for rel in (1, 3, 2):
                xm_copy(rel, pair, phase).start()
            return carry

        if with_mix:
            lax.fori_loop(0, 8, go_mix, 0)

    def d_span(phase):
        group, octet, until, with_mix = PHASES[phase]
        first_row, last_row = 32 * octet, 80 if with_mix else 32 * until
        return pl.ds(STARTS[group], GROUPS[group]), first_row, last_row - first_row

    def d_copy(phase, device, other):
        span, row, count = d_span(phase)
        src = dall.at[other, span, pl.ds(row, count)]
        place = pl.ds(pl.multiple_of(plane * 80 + row, 8), count)
        if PHASES[phase][0] == LAST:
            dst = ylast.at[:, place, :]
        else:
            dst = yall.at[span, place, :]
        if device is None:
            return pltpu.make_async_copy(src, dst, dl_sem.at[phase])
        return pltpu.make_async_remote_copy(
            src_ref=src,
            dst_ref=dst,
            send_sem=ds_sem.at[phase],
            recv_sem=dr_sem.at[phase],
            device_id=device,
            device_id_type=MESH,
        )

    def d_wait(phase, sem):
        span, row, count = d_span(phase)
        whole = dall.at[pl.ds(0, 15), span, pl.ds(row, count)]
        pltpu.make_async_copy(whole, whole, sem.at[phase]).wait()

    def turn(phase):
        group, first_octet, until, with_mix = PHASES[phase]
        i0, count = STARTS[group], GROUPS[group]

        def go(r, carry):
            i, place = i0 + r // 16, r % 16
            other = lo * place + (1 - lo) * (15 - place)

            def put(octet, offset, near_value, far_value):
                pitch, base = (16, 16, 8)[octet], 32 * octet + offset
                dall[other, i, pl.ds(pl.multiple_of(lo * pitch + base, 8), 8), :] = near_value
                dall[other, i, pl.ds(pl.multiple_of((1 - lo) * pitch + base, 8), 8), :] = far_value

            for octet in range(first_octet, until):
                for part in range(2):
                    base = octet * 8 * PITCH + 32 * i0 + part * 16 * count + r

                    def take(ref, item):
                        return ref[pl.ds(item * 16 * PITCH + base, 8, stride=PITCH), :]

                    put(octet, part * 8, take(xs, own) + take(xr, 1), take(xr, 0) + take(xr, 2))

            def take_mix(ref, item):
                return ref[pl.ds(item * 8 * MIX_PITCH + 16 * i0 + r, 8, stride=MIX_PITCH), :]

            if with_mix:
                put(2, 0, take_mix(xsm, own) + take_mix(xrm, 1), take_mix(xrm, 0) + take_mix(xrm, 2))
            return carry

        lax.fori_loop(0, 16 * count, go, 0)

    def x_wait(phase, sem):
        group, octet, until, with_mix = PHASES[phase]
        main = xr.at[pl.ds(0, 256 * (until - octet) * GROUPS[group]), :]
        mix = xrm.at[pl.ds(0, 128 * GROUPS[group]), :]
        for rel in range(3):
            if until > octet:
                pltpu.make_async_copy(main, main, sem.at[0, rel, phase]).wait()
            if with_mix:
                pltpu.make_async_copy(mix, mix, sem.at[1, rel, phase]).wait()

    lines = fields.reshape(24576, 128)

    def y_load(i):
        return pltpu.make_async_copy(
            yall.at[i], lines.at[pl.ds(pl.multiple_of(i * 1280, 1280), 1280), :], y_sem.at[i]
        )

    def part_copy(i):
        return pltpu.make_async_copy(rows.at[i % 2], parts.at[i], p_sem.at[i])

    def second(group):
        for phase in range(len(PHASES)):
            if PHASES[phase][0] == group:
                d_wait(phase, dr_sem)
                d_copy(phase, None, plane).wait()
        first_i, last_i = STARTS[group], STARTS[group] + GROUPS[group]
        if group < LAST:
            for i in range(first_i, last_i):
                y_load(i).start()

        def go(i, carry):
            if group < LAST:
                y_load(i).wait()

            @pl.when(i >= 2)
            def _():
                part_copy(i - 2).wait()

            def lift(offsets):
                return jnp.concatenate(
                    [
                        lines[pl.ds(pl.multiple_of(i * 1280 + 80 * j + offset, 8), 8), :]
                        if group < LAST
                        else ylast[0, 80 * j + offset : 80 * j + offset + 8, :]
                        for j in range(16)
                        for offset in offsets
                    ],
                    axis=0,
                )

            second_rows(lift, fth, ftl, rows.at[i % 2], slab * 10 + i)
            part_copy(i).start()
            return carry

        lax.fori_loop(first_i, last_i, go, 0)

    for phase in range(len(PHASES)):
        if phase + 1 < len(PHASES):
            send_x(phase + 1)
        x_wait(phase, xr_sem)
        turn(phase)
        for step in STEPS:
            other, device = peer_plane(step)
            d_copy(phase, device, other).start()
        d_copy(phase, None, plane).start()
        if phase == 0:
            for table in tables[6:]:
                table.wait()
        elif 2 <= phase <= LAST + 1:
            second(phase - 2)

    second(LAST)

    def z_left(chunk, carry):
        z_copy(chunk).wait_send()
        return carry

    lax.fori_loop(12, 16, z_left, 0)
    lax.fori_loop(22, 24, z_left, 0)
    for phase in range(len(PHASES)):
        x_wait(phase, xs_sem)
    for phase in range(len(PHASES)):
        d_wait(phase, ds_sem)
    part_copy(8).wait()
    part_copy(9).wait()


def exchange(u, v, t):
    zh, zl = depth_tables()
    xh, xl = first_tables()
    fh, fl = second_tables()
    phases = len(PHASES)
    any_space = pl.BlockSpec(memory_space=pl.ANY)
    return pl.pallas_call(
        exchange_kernel,
        out_shape=(
            jax.ShapeDtypeStruct((9, 1280, 128), F32),
            jax.ShapeDtypeStruct((10, 3, 320, 128), F32),
        ),
        in_specs=[any_space] * 9,
        out_specs=(any_space, any_space),
        scratch_shapes=[
            pltpu.VMEM((3, 4, 2, 128, 8, 128), F32),
            pltpu.VMEM((3, 512, 256), BF16),
            pltpu.VMEM((3, 512, 256), BF16),
            pltpu.VMEM((352, 256), BF16),
            pltpu.VMEM((352, 256), BF16),
            pltpu.VMEM((2, 2, 320, 256), BF16),
            pltpu.VMEM((2, 2, 320, 256), BF16),
            pltpu.VMEM((1024, 512), BF16),
            pltpu.VMEM((512, 256), F32),
            pltpu.VMEM((24, 2, 256, 256), F32),
            pltpu.VMEM((6, 2, 128, 256), F32),
            pltpu.VMEM((4 * 16 * PITCH, 128), F32),
            pltpu.VMEM((3 * 16 * PITCH, 128), F32),
            pltpu.VMEM((4 * 8 * MIX_PITCH, 128), F32),
            pltpu.VMEM((3 * 8 * MIX_PITCH, 128), F32),
            pltpu.VMEM((16, 10, 80, 128), F32),
            pltpu.VMEM((1, 1280, 128), F32),
            pltpu.VMEM((2, 3, 320, 128), F32),
            pltpu.SemaphoreType.DMA((2, 3, 4)),
            pltpu.SemaphoreType.DMA((8,)),
            pltpu.SemaphoreType.DMA((24,)),
            pltpu.SemaphoreType.DMA((24,)),
            pltpu.SemaphoreType.DMA((2, 3, phases)),
            pltpu.SemaphoreType.DMA((2, 3, phases)),
            pltpu.SemaphoreType.DMA((phases,)),
            pltpu.SemaphoreType.DMA((phases,)),
            pltpu.SemaphoreType.DMA((phases,)),
            pltpu.SemaphoreType.DMA((10,)),
            pltpu.SemaphoreType.DMA((10,)),
        ],
        compiler_params=pltpu.CompilerParams(
            collective_id=0, has_side_effects=True, vmem_limit_bytes=67043328
        ),
        name="exchange",
    )(u, v, t, zh, zl, xh, xl, fh, fl)


def lay_out_kernel(parts, out):
    for i in range(5):
        out[0, i, :, :128] = parts[i, 0]
        out[0, i, :, 128:256] = parts[i, 1]
        out[0, i, :, 256:] = parts[i, 2, :, :64]


def lay_out(parts):
    return pl.pallas_call(
        lay_out_kernel,
        grid=(2,),
        out_shape=jax.ShapeDtypeStruct((1, 10, 320, 320), F32),
        in_specs=[pl.BlockSpec((5, 3, 320, 128), lambda i: (i, 0, 0, 0))],
        out_specs=pl.BlockSpec((1, 5, 320, 320), lambda i: (0, i, 0, 0)),
        compiler_params=pltpu.CompilerParams(dimension_semantics=("arbitrary",)),
        name="lay_out",
    )(parts)


def shards(velocity_u, velocity_v, scalar_theta):
    return lay_out(exchange(velocity_u, velocity_v, scalar_theta)[1])


def solution(mesh):
    spec = P("field", "slab", None)
    return jax.shard_map(
        shards,
        mesh=mesh,
        in_specs=(spec, spec, spec),
        out_specs=P("field", "slab", None, None),
        check_vma=False,
    )
```
